256 devices in a mesh: band: 64 (over z, y, core), field: 4 (over x).
Axes of the slice: x: 4, y: 4, z: 8, core: 2. Of those that a mesh axis runs over, the one named last changes fastest.
Arguments:
- right_side: float32 [640, 2, 4, 12, 640], P('band', None, 'field'), may hold values from -40 to 40
- legendre: bfloat16 [640, 640, 640], P('band'), may hold values from -0.25 to 0.25
- wave_map: int32 [640], replicated, may hold values from 0 to 639, as said below
- obs_weight: float32 [640, 1280], P('band'), may hold values from 0.2 to 5
Outputs:
- solution: float32 [640, 2, 4, 12, 640], P('band', None, 'field')
- residual: float32 [640, 2, 4, 12, 640], P('band', None, 'field')
The draws below stay inside these ranges and needn't reach their ends.
Inputs may be any that keep to these rules, and one draw needn't show every extreme that they name: A permutation of 0 to 639; wave_map[s] lies in the same aligned block of 20 values as 639-s.
All inputs are finite; a program needn't handle non-finite values.
Results may differ from the reference program's by a relative error of at most 0.03.
Values may be sent and summed in bfloat16 or wider, within the bound.
No kernel may reach another device: no remote copies, remote signals or barrier semaphores. Data moves between devices by JAX's collectives and lax.ppermute only.
A program may use at most 128 MiB of HBM per device.

```python
import math
import jax
import jax.numpy as jnp
from jax import lax

MW = 640
NLAT = 640
NLON = 1280
FIELDS = 4
LEV = 12
ITERS = 3


def draw_right_side(key, part):
    first_key, second_key = jax.random.split(key, 2)
    shape = (MW, 2, FIELDS, LEV, MW)
    base = jax.random.normal(first_key, shape, jnp.float32)
    scales = jnp.exp(jax.random.uniform(second_key, (1, 1, FIELDS, LEV, 1), jnp.float32, 0.0, math.log(10.0)))
    return jnp.clip(base * scales, -40.0, 40.0)


def shuffle_block(block_key):
    return jax.random.permutation(block_key, MW // 32)


def draw_wave_map(key, part):
    block_width = MW // 32
    subkeys = jax.random.split(key, 32)
    shuffled = jax.vmap(shuffle_block)(subkeys).astype(jnp.int32)
    starts = jnp.arange(32, dtype=jnp.int32)[:, None] * block_width
    return (MW - 1 - (starts + shuffled)).reshape(MW).astype(jnp.int32)


def steps_of(stream_key, extent, cuts, smallest, top_value):
    def one(axis_at, parts):
        draws = jax.random.uniform(jax.random.fold_in(jax.random.fold_in(stream_key, 6), axis_at), (parts,), jnp.float32, smallest / len(cuts), top_value / len(cuts))
        return jnp.repeat(jnp.exp(draws), extent[axis_at] // parts).reshape((-1,) + (1,) * (len(extent) - axis_at - 1))

    factor_of = one(*cuts[0])
    for cut in cuts[1:]:
        factor_of = factor_of * one(*cut)
    return factor_of


def centred(rng, shape, deviation, most, pieces=(), held_as=jnp.bfloat16):
    drawn = jax.random.normal(rng, shape, jnp.float32) * deviation
    if len(pieces) > 0:
        drawn = steps_of(rng, shape, pieces, -0.22, 0.18) * drawn
    return jnp.clip(drawn, min=-most, max=most).astype(held_as)


def setup_inputs(seed: int = 0) -> dict:
    splits = jax.random.split(jax.random.key(seed), 5)
    right_side = draw_right_side(jax.random.fold_in(splits[4], 71), 0)
    legendre = centred(splits[1], (MW, MW, NLAT), MW ** -0.5, 0.25, ((0, 64),))
    wave_map = draw_wave_map(jax.random.fold_in(splits[4], 71), 0)
    obs_weight = jnp.clip(jnp.exp(math.log(5.0) - 3.218876 * jax.random.uniform(splits[3], (NLAT, NLON), jnp.float32) ** steps_of(splits[3], (NLAT, NLON), ((0, 64),), -0.2, 0.2)), 0.2, 5.0)
    return {"right_side": right_side, "legendre": legendre, "wave_map": wave_map, "obs_weight": obs_weight}


def triangle_of(own_waves, degrees):
    return (jnp.arange(degrees, dtype=jnp.int32)[None, :] >= own_waves[:, None]).astype(jnp.float32)

def fourier_of(wave_map, lon_count):
    longitude = jnp.arange(lon_count, dtype=jnp.int32)
    phase_int = wave_map[:, None].astype(jnp.int32) * longitude[None, :] % lon_count
    angles = phase_int.astype(jnp.float32) * (2.0 * math.pi / lon_count)
    norm_factor = 1.0 / math.sqrt(wave_map.shape[0])
    return (jnp.stack([jnp.cos(angles), -jnp.sin(angles)], axis=1) * norm_factor).astype(jnp.bfloat16)

def operate(vector, legendre, fourier_table, triangle, obs_weight):
    masked_bf = (vector * triangle[:, None, None, None, :]).astype(jnp.bfloat16)
    coeffs = lax.dot_general(masked_bf, legendre, (((4,), (1,)), ((0,), (0,))), preferred_element_type=jnp.float32).astype(jnp.bfloat16)
    grid_vals = lax.dot_general(coeffs, fourier_table, (((0, 1), (0, 1)), ((), ())), preferred_element_type=jnp.float32)
    weighted = (grid_vals * obs_weight).astype(jnp.bfloat16)
    returned = lax.dot_general(fourier_table, weighted, (((2,), (3,)), ((), ())), preferred_element_type=jnp.float32).astype(jnp.bfloat16)
    adjoint = lax.dot_general(returned, legendre, (((4,), (2,)), ((0,), (0,))), preferred_element_type=jnp.float32)
    return vector + triangle[:, None, None, None, :] * adjoint

def reference(right_side, legendre, wave_map, obs_weight):
    triangle = triangle_of(wave_map, right_side.shape[4])
    fourier_table = fourier_of(wave_map, obs_weight.shape[1])
    residual = right_side * triangle[:, None, None, None, :]
    direction = residual
    solution = jnp.zeros_like(residual)
    norm_now = jnp.sum(residual * residual)
    for iteration in range(ITERS):
        image_vec = operate(direction, legendre, fourier_table, triangle, obs_weight)
        step_length = norm_now / jnp.sum(direction * image_vec)
        solution = solution + step_length * direction
        residual = residual - step_length * image_vec
        norm_next = jnp.sum(residual * residual)
        direction = residual + norm_next / norm_now * direction
        norm_now = norm_next
    return (solution, residual)
```

```python
import functools
import math

import jax
import jax.numpy as jnp
from jax import lax
from jax.experimental import pallas as pl
from jax.experimental.pallas import tpu as pltpu
from jax.sharding import Mesh
from jax.sharding import PartitionSpec as P

ZS, YS, CS, XS = 8, 4, 2, 4
BAND = ("z", "y", "c")
EXCHANGE = ("z", "c", "y")
GROUPS = 3
PIECE = 40
PIECES = 16
SUB = 8
LANES = 128
SPARE = GROUPS * PIECE
F32 = jnp.float32
BF16 = jnp.bfloat16


def lane_of(rows=SUB):
    return lax.broadcasted_iota(jnp.int32, (rows, LANES), 1)


def scatter_rows(value, acc_ref, slot, chunk_rows, slots):
    lane = lane_of()
    for piece in range(PIECES):
        first = piece * PIECE
        tile, offset = first // LANES, first % LANES
        out = jnp.zeros((SUB, LANES), F32)
        for group in reversed(range(GROUPS)):
            rows = slice(group * SUB, (group + 1) * SUB)
            source = value[rows, tile * LANES : (tile + 1) * LANES]
            if offset + PIECE > LANES:
                following = value[rows, (tile + 1) * LANES : (tile + 2) * LANES]
                source = jnp.where(lane >= offset, source, following)
            shift = (group * PIECE - offset) % LANES
            if shift:
                source = pltpu.roll(source, shift, 1)
            out = jnp.where(lane < (group + 1) * PIECE, source, out)
        acc_ref[pl.ds(piece * YS * chunk_rows + slot, SUB, stride=slots), :] = out


def gather_rows(held_ref, slot, chunk_rows, slots, lat_tiles):
    lane = lane_of()
    tiles = [[None] * lat_tiles for _ in range(GROUPS)]
    for piece in range(PIECES):
        first = piece * PIECE
        tile, offset = first // LANES, first % LANES
        rows = held_ref[pl.ds(piece * YS * chunk_rows + slot, SUB, stride=slots), :]
        for group in range(GROUPS):
            shift = (offset - group * PIECE) % LANES
            moved = pltpu.roll(rows, shift, 1) if shift else rows
            known = tiles[group][tile]
            tiles[group][tile] = moved if known is None else jnp.where(lane >= offset, moved, known)
            if offset + PIECE > LANES:
                tiles[group][tile + 1] = moved
    return jnp.concatenate([jnp.concatenate(row, axis=1) for row in tiles], axis=0)


def square_sum(parts):
    total = None
    for part in parts:
        for group in range(GROUPS):
            block = part[group * SUB : (group + 1) * SUB, :]
            total = block * block if total is None else total + block * block
    return total


def triangle_tile(wave, tile):
    return lane_of(GROUPS * SUB) + tile * LANES >= wave


def first_kernel(slots, chunk_rows, waves_ref, vec_ref, leg_ref, res_ref, out_ref, norm_ref, acc_ref):
    slot = pl.program_id(0)
    wave = waves_ref[slot]
    tiles = vec_ref.shape[2] // LANES
    parts = []
    for tile in range(tiles):
        cols = slice(tile * LANES, (tile + 1) * LANES)
        parts.append(jnp.where(triangle_tile(wave, tile), vec_ref[0, :, cols], 0.0))
        res_ref[0, :, cols] = parts[-1]

    @pl.when(slot == 0)
    def _():
        norm_ref[...] = jnp.zeros_like(norm_ref)

    norm_ref[...] += square_sum(parts)
    forward(jnp.concatenate(parts, axis=1), leg_ref, acc_ref, out_ref, slot, slots, chunk_rows)


def forward(vector, leg_ref, acc_ref, out_ref, slot, slots, chunk_rows):
    coeffs = jnp.dot(vector.astype(BF16), leg_ref[0], preferred_element_type=F32)
    scatter_rows(coeffs, acc_ref, slot, chunk_rows, slots)

    @pl.when(slot == slots - 1)
    def _():
        out_ref[...] = acc_ref[...].astype(BF16)


def sums_of(sum_refs, chunk_rows):
    total = sum_refs[0][...]
    for ref in sum_refs[1:]:
        total = total + ref[...]
    total = total * (1.0 / chunk_rows)
    lane = lane_of()
    norm = jnp.sum(jnp.where((lane >= SPARE) & (lane < SPARE + 3), total, 0.0), axis=(0, 1), keepdims=True)
    energy = jnp.sum(jnp.where((lane >= SPARE + 3) & (lane < SPARE + 6), total, 0.0), axis=(0, 1), keepdims=True)
    return norm, norm + energy


def image_of(vec_refs, held_ref, leg_ref, wave, slot, slots, chunk_rows):
    tiles = leg_ref.shape[2] // LANES
    home = gather_rows(held_ref, slot, chunk_rows, slots, tiles).astype(BF16)
    adjoint = lax.dot_general(home, leg_ref[0], (((1,), (1,)), ((), ())), preferred_element_type=F32)
    image = []
    for tile in range(leg_ref.shape[1] // LANES):
        cols = slice(tile * LANES, (tile + 1) * LANES)
        image.append(vec_refs[0, :, cols] + jnp.where(triangle_tile(wave, tile), adjoint[:, cols], 0.0))
    return image


def scalar_row(value):
    return jnp.broadcast_to(value, (1, LANES))


def middle_kernel(stage, slots, chunk_rows, *refs):
    waves_ref, home_ref, leg_ref, sum_a, sum_b, sum_c, sum_d, past_ref, *refs = refs
    if stage == 0:
        res_ref, new_ref, along_ref, out_ref, norm_ref, hist_ref, acc_ref, held_ref = refs
    else:
        res_ref, last_ref, new_ref, along_ref, out_ref, norm_ref, hist_ref, acc_ref, held_ref = refs
    slot = pl.program_id(0)
    wave = waves_ref[slot]

    @pl.when(slot == 0)
    def _():
        held_ref[...] = home_ref[...].astype(F32)
        norm, product = sums_of((sum_a, sum_b, sum_c, sum_d), chunk_rows)
        hist_ref[...] = jnp.zeros_like(hist_ref)
        if stage == 0:
            alpha = norm / product
            beta = jnp.zeros_like(norm)
            hist_ref[2:3, :] = scalar_row(alpha)
        else:
            beta = norm / past_ref[0:1, 0:1]
            alpha = norm / (product - beta * norm / past_ref[1:2, 0:1])
            hist_ref[2:3, :] = past_ref[2:3, :]
            hist_ref[3:4, :] = scalar_row(alpha)
        hist_ref[0:1, :] = scalar_row(norm)
        hist_ref[1:2, :] = scalar_row(alpha)
        hist_ref[4:5, :] = scalar_row(beta)
        norm_ref[...] = jnp.zeros_like(norm_ref)

    alpha = hist_ref[1:2, :]
    beta = hist_ref[4:5, :]
    image = image_of(res_ref, held_ref, leg_ref, wave, slot, slots, chunk_rows)
    parts = []
    for tile, along in enumerate(image):
        cols = slice(tile * LANES, (tile + 1) * LANES)
        if stage > 0:
            along = along + beta * last_ref[0, :, cols]
        along_ref[0, :, cols] = along
        part = res_ref[0, :, cols] - alpha * along
        new_ref[0, :, cols] = part
        parts.append(part)
    norm_ref[...] += square_sum(parts)
    forward(jnp.concatenate(parts, axis=1), leg_ref, acc_ref, out_ref, slot, slots, chunk_rows)


def last_kernel(slots, chunk_rows, *refs):
    waves_ref, home_ref, leg_ref, sum_a, sum_b, sum_c, sum_d, past_ref, *refs = refs
    res0_ref, res1_ref, res2_ref, last_ref, sol_ref, fin_ref, hist_ref, held_ref = refs
    slot = pl.program_id(0)
    wave = waves_ref[slot]

    @pl.when(slot == 0)
    def _():
        held_ref[...] = home_ref[...].astype(F32)
        norm, product = sums_of((sum_a, sum_b, sum_c, sum_d), chunk_rows)
        beta = norm / past_ref[0:1, 0:1]
        alpha = norm / (product - beta * norm / past_ref[1:2, 0:1])
        hist_ref[0:1, :] = scalar_row(alpha)
        hist_ref[1:2, :] = scalar_row(beta)

    alpha = hist_ref[0:1, :]
    beta = hist_ref[1:2, :]
    alpha0, alpha1, beta1 = past_ref[2:3, :], past_ref[3:4, :], past_ref[4:5, :]
    image = image_of(res2_ref, held_ref, leg_ref, wave, slot, slots, chunk_rows)
    for tile, along in enumerate(image):
        cols = slice(tile * LANES, (tile + 1) * LANES)
        along = along + beta * last_ref[0, :, cols]
        res2 = res2_ref[0, :, cols]
        fin_ref[0, :, cols] = res2 - alpha * along
        first = res0_ref[0, :, cols]
        second = res1_ref[0, :, cols] + beta1 * first
        third = res2 + beta * second
        sol_ref[0, :, cols] = alpha0 * first + alpha1 * second + alpha * third


def fourier_kernel(chunk_rows, slots, norm_factor, lon_count, waves_ref, out_ref):
    rows = waves_ref.shape[0]
    wave = waves_ref[...].astype(F32)
    lane = lax.broadcasted_iota(jnp.int32, (rows, LANES), 1).astype(F32)
    row = lax.broadcasted_iota(jnp.int32, (rows, LANES), 0) + pl.program_id(0) * rows
    within = row - (row // chunk_rows) * chunk_rows
    quarter = jnp.where(within >= slots, 0.25 * lon_count, 0.0)
    fine_cos, fine_sin = turn(wave * lane, lon_count)
    coarse_cos, coarse_sin = turn(wave * (lane * LANES) + quarter, lon_count)
    coarse_cos = coarse_cos * norm_factor
    coarse_sin = coarse_sin * norm_factor
    for tile in range(lon_count // LANES):
        value = coarse_cos[:, tile : tile + 1] * fine_cos - coarse_sin[:, tile : tile + 1] * fine_sin
        out_ref[:, tile * LANES : (tile + 1) * LANES] = value.astype(BF16)


def turn(phase, period):
    phase = phase - period * jnp.floor(phase * (1.0 / period) + 0.5)
    quadrant = jnp.floor(phase * (4.0 / period) + 0.5)
    angle = (phase - quadrant * (0.25 * period)) * (2.0 * math.pi / period)
    sq = angle * angle
    cosine = 1.0 + sq * (-1.0 / 2 + sq * (1.0 / 24 + sq * (-1.0 / 720 + sq * (1.0 / 40320))))
    sine = angle * (1.0 + sq * (-1.0 / 6 + sq * (1.0 / 120 + sq * (-1.0 / 5040 + sq * (1.0 / 362880)))))
    odd = jnp.abs(quadrant) == 1.0
    cos_base = jnp.where(odd, -quadrant * sine, cosine)
    sin_base = jnp.where(odd, quadrant * cosine, sine)
    back = jnp.abs(quadrant) == 2.0
    return jnp.where(back, -cos_base, cos_base), jnp.where(back, -sin_base, sin_base)


def pieces_of(value):
    high = value.astype(BF16).astype(F32)
    middle = (value - high).astype(BF16).astype(F32)
    low = (value - high - middle).astype(BF16).astype(F32)
    return high, middle, low


def grid_kernel(x_ref, table_ref, weight_ref, norm_ref, out_ref, turned_ref, wide_ref):
    count, lons = table_ref.shape
    step = 256
    turned_ref[...] = x_ref[...].astype(F32).T.astype(BF16)
    energy = jnp.zeros((SUB, step), F32)
    for first in range(0, lons, step):
        cols = slice(first, first + step)
        grid = jnp.dot(turned_ref[...], table_ref[:, cols], preferred_element_type=F32)
        weight = weight_ref[:, cols]
        weighted = []
        for group in range(GROUPS):
            rows = grid[group * PIECE : (group + 1) * PIECE]
            product = weight * rows
            weighted.append(product)
            square = product * rows
            for block in range(0, PIECE, SUB):
                energy = energy + square[block : block + SUB]
        weighted.append(jnp.zeros((LANES - SPARE, step), F32))
        wide_ref[cols, :] = jnp.concatenate(weighted, axis=0).T.astype(BF16)
    lane = lane_of(1)
    spare = jnp.zeros((1, LANES), F32)
    values = pieces_of(jnp.sum(norm_ref[...], axis=(0, 1), keepdims=True))
    values = values + pieces_of(jnp.sum(energy, axis=(0, 1), keepdims=True))
    for place, value in enumerate(values):
        spare = jnp.where(lane == SPARE + place, value, spare)
    for first in range(0, count, step):
        rows = slice(first, first + step)
        back = jnp.dot(table_ref[rows, :], wide_ref[...], preferred_element_type=F32)
        out_ref[rows, :] = jnp.where(lane >= SPARE, spare, back).astype(BF16)


def tail_kernel(x_ref, out_ref):
    total = jnp.zeros((SUB, LANES), F32)
    block = 2 * SUB
    for first in range(0, x_ref.shape[0], block):
        value = x_ref[first : first + block, :].astype(F32)
        total = total + value[:SUB] + value[SUB:]
    out_ref[...] = total


def exchange(payload, parts):
    rows = payload.shape[0]
    packed = payload.reshape(parts, rows // parts // 2, 2, LANES)
    return lax.all_to_all(packed, EXCHANGE, 0, 0, tiled=True).reshape(rows, LANES)


def whole(shape):
    return pl.BlockSpec(shape, lambda *_: (0,) * len(shape))


def on_device(right_side, legendre, wave_map, obs_weight):
    slots, degrees, lats = legendre.shape
    lon_count = obs_weight.shape[1]
    bands = ZS * YS * CS
    rows = bands * 2 * slots
    chunk_rows = 2 * slots
    band_at = lax.axis_index(BAND)
    own_waves = lax.dynamic_slice_in_dim(wave_map, band_at * slots, slots)

    vec = right_side.reshape(slots, 2, GROUPS, YS, degrees).transpose(0, 2, 3, 1, 4)
    vec = vec.reshape(slots, GROUPS * SUB, degrees)

    spread = wave_map.reshape(ZS, YS, CS, slots).transpose(0, 2, 1, 3).reshape(bands, 1, slots)
    spread = jnp.broadcast_to(spread, (bands, 2, slots)).reshape(rows, 1)
    spread = jnp.broadcast_to(spread, (rows, LANES))
    block = 128
    table = pl.pallas_call(
        functools.partial(fourier_kernel, chunk_rows, slots, 1.0 / math.sqrt(wave_map.shape[0]), lon_count),
        grid=(rows // block,),
        in_specs=[pl.BlockSpec((block, LANES), lambda i: (i, 0))],
        out_specs=pl.BlockSpec((block, lon_count), lambda i: (i, 0)),
        out_shape=jax.ShapeDtypeStruct((rows, lon_count), BF16),
        cost_estimate=pl.CostEstimate(flops=4_000_000_000, bytes_accessed=4_000_000, transcendentals=0),
        name="fourier",
    )(spread)

    near = jnp.broadcast_to(obs_weight[None], (YS * CS,) + obs_weight.shape)
    near = lax.all_to_all(near, ("y", "c"), 0, 0, tiled=True)
    near = lax.dynamic_slice_in_dim(near, lax.axis_index("c") * YS, YS)
    weight = near.reshape(PIECE, lon_count)

    slot_block = pl.BlockSpec((1, GROUPS * SUB, degrees), lambda i: (i, 0, 0))
    leg_block = pl.BlockSpec((1, degrees, lats), lambda i: (i, 0, 0))
    smem = pl.BlockSpec(memory_space=pltpu.SMEM)
    small = whole((SUB, LANES))
    payload_block = whole((rows, LANES))
    vec_shape = jax.ShapeDtypeStruct((slots, GROUPS * SUB, degrees), F32)
    payload_shape = jax.ShapeDtypeStruct((rows, LANES), BF16)
    small_shape = jax.ShapeDtypeStruct((SUB, LANES), F32)
    held = pltpu.VMEM((rows, LANES), F32)
    cost = pl.CostEstimate(flops=4_000_000_000, bytes_accessed=9_000_000, transcendentals=0)

    res, payload, norm = pl.pallas_call(
        functools.partial(first_kernel, slots, chunk_rows),
        grid=(slots,),
        in_specs=[smem, slot_block, leg_block],
        out_specs=[slot_block, payload_block, small],
        out_shape=[vec_shape, payload_shape, small_shape],
        scratch_shapes=[held],
        cost_estimate=cost,
        name="first",
    )(own_waves, vec, legendre)

    def reach(payload, norm):
        arrived = exchange(payload, bands)
        back = pl.pallas_call(
            grid_kernel,
            out_shape=payload_shape,
            scratch_shapes=[pltpu.VMEM((LANES, rows), BF16), pltpu.VMEM((lon_count, LANES), BF16)],
            cost_estimate=cost,
            name="grid",
        )(arrived, table, weight, norm)
        home = exchange(back, bands)
        sums = pl.pallas_call(
            tail_kernel,
            out_shape=small_shape,
            name="tail",
        )(home)
        others = [lax.ppermute(sums, "x", [(i, (i + k) % XS) for i in range(XS)]) for k in range(1, XS)]
        return home, [sums] + others

    past = jnp.zeros((SUB, LANES), F32)
    residuals = [res]
    along = None
    for stage in range(2):
        home, sums = reach(payload, norm)
        operands = [own_waves, home, legendre, *sums, past, residuals[-1]]
        specs = [smem, payload_block, leg_block, small, small, small, small, small, slot_block]
        if stage > 0:
            operands.append(along)
            specs.append(slot_block)
        res, along, payload, norm, past = pl.pallas_call(
            functools.partial(middle_kernel, stage, slots, chunk_rows),
            grid=(slots,),
            in_specs=specs,
            out_specs=[slot_block, slot_block, payload_block, small, small],
            out_shape=[vec_shape, vec_shape, payload_shape, small_shape, small_shape],
            scratch_shapes=[held, held],
            cost_estimate=cost,
            name=f"middle{stage}",
        )(*operands)
        residuals.append(res)
    home, sums = reach(payload, norm)
    solution, residual = pl.pallas_call(
        functools.partial(last_kernel, slots, chunk_rows),
        grid=(slots,),
        in_specs=[smem, payload_block, leg_block, small, small, small, small, small] + [slot_block] * 4,
        out_specs=[slot_block, slot_block],
        out_shape=[vec_shape, vec_shape],
        scratch_shapes=[pltpu.VMEM((SUB, LANES), F32), held],
        cost_estimate=cost,
        name="last",
    )(own_waves, home, legendre, *sums, past, *residuals, along)

    def unpack(value):
        value = value.reshape(slots, GROUPS, YS, 2, degrees).transpose(0, 3, 1, 2, 4)
        return value.reshape(right_side.shape)

    return unpack(solution), unpack(residual)


def solution(mesh):
    split = Mesh(mesh.devices.reshape(ZS, YS, CS, XS), ("z", "y", "c", "x"))
    return jax.shard_map(
        on_device,
        mesh=split,
        in_specs=(P(BAND, None, "x", None, None), P(BAND, None, None), P(), P(BAND, None)),
        out_specs=(P(BAND, None, "x", None, None), P(BAND, None, "x", None, None)),
        check_vma=False,
    )
```

```python
import functools
import math

import jax
import jax.numpy as jnp
from jax import lax
from jax.experimental import pallas as pl
from jax.experimental.pallas import tpu as pltpu
from jax.sharding import Mesh
from jax.sharding import PartitionSpec as P

ZS, YS, CS, XS = 8, 4, 2, 4
BAND = ("z", "y", "c")
EXCHANGE = ("z", "c", "y")
GROUPS = 3
PIECE = 40
PIECES = 16
SUB = 8
LANES = 128
SPARE = GROUPS * PIECE
F32 = jnp.float32
BF16 = jnp.bfloat16


def lane_of(rows=SUB):
    return lax.broadcasted_iota(jnp.int32, (rows, LANES), 1)


def scatter_rows(value, acc_ref, slot, chunk_rows, slots):
    lane = lane_of()
    for piece in range(PIECES):
        first = piece * PIECE
        tile, offset = first // LANES, first % LANES
        out = jnp.zeros((SUB, LANES), F32)
        for group in reversed(range(GROUPS)):
            rows = slice(group * SUB, (group + 1) * SUB)
            source = value[rows, tile * LANES : (tile + 1) * LANES]
            if offset + PIECE > LANES:
                following = value[rows, (tile + 1) * LANES : (tile + 2) * LANES]
                source = jnp.where(lane >= offset, source, following)
            shift = (group * PIECE - offset) % LANES
            if shift:
                source = pltpu.roll(source, shift, 1)
            out = jnp.where(lane < (group + 1) * PIECE, source, out)
        acc_ref[pl.ds(piece * YS * chunk_rows + slot, SUB, stride=slots), :] = out


def gather_rows(held_ref, slot, chunk_rows, slots, lat_tiles):
    lane = lane_of()
    tiles = [[None] * lat_tiles for _ in range(GROUPS)]
    for piece in range(PIECES):
        first = piece * PIECE
        tile, offset = first // LANES, first % LANES
        rows = held_ref[pl.ds(piece * YS * chunk_rows + slot, SUB, stride=slots), :]
        for group in range(GROUPS):
            shift = (offset - group * PIECE) % LANES
            moved = pltpu.roll(rows, shift, 1) if shift else rows
            known = tiles[group][tile]
            tiles[group][tile] = moved if known is None else jnp.where(lane >= offset, moved, known)
            if offset + PIECE > LANES:
                tiles[group][tile + 1] = moved
    return jnp.concatenate([jnp.concatenate(row, axis=1) for row in tiles], axis=0)


def square_sum(parts):
    total = None
    for part in parts:
        for group in range(GROUPS):
            block = part[group * SUB : (group + 1) * SUB, :]
            total = block * block if total is None else total + block * block
    return total


def triangle_tile(wave, tile):
    return lane_of(GROUPS * SUB) + tile * LANES >= wave


def first_kernel(slots, chunk_rows, waves_ref, vec_ref, leg_ref, res_ref, out_ref, norm_ref, acc_ref):
    slot = pl.program_id(0)
    wave = waves_ref[slot]
    tiles = vec_ref.shape[2] // LANES
    parts = []
    for tile in range(tiles):
        cols = slice(tile * LANES, (tile + 1) * LANES)
        parts.append(jnp.where(triangle_tile(wave, tile), vec_ref[0, :, cols], 0.0))
        res_ref[0, :, cols] = parts[-1]

    @pl.when(slot == 0)
    def _():
        norm_ref[...] = jnp.zeros_like(norm_ref)

    norm_ref[...] += square_sum(parts)
    forward(jnp.concatenate(parts, axis=1), leg_ref, acc_ref, out_ref, slot, slots, chunk_rows)


def forward(vector, leg_ref, acc_ref, out_ref, slot, slots, chunk_rows):
    coeffs = jnp.dot(vector.astype(BF16), leg_ref[0], preferred_element_type=F32)
    scatter_rows(coeffs, acc_ref, slot, chunk_rows, slots)

    @pl.when(slot == slots - 1)
    def _():
        out_ref[...] = acc_ref[...].astype(BF16)


def sums_of(sum_refs, chunk_rows):
    total = sum_refs[0][...]
    for ref in sum_refs[1:]:
        total = total + ref[...]
    total = total * (1.0 / chunk_rows)
    lane = lane_of()
    norm = jnp.sum(jnp.where((lane >= SPARE) & (lane < SPARE + 3), total, 0.0), axis=(0, 1), keepdims=True)
    energy = jnp.sum(jnp.where((lane >= SPARE + 3) & (lane < SPARE + 6), total, 0.0), axis=(0, 1), keepdims=True)
    return norm, norm + energy


def image_of(vec_refs, held_ref, leg_ref, wave, slot, slots, chunk_rows):
    tiles = leg_ref.shape[2] // LANES
    home = gather_rows(held_ref, slot, chunk_rows, slots, tiles).astype(BF16)
    adjoint = lax.dot_general(home, leg_ref[0], (((1,), (1,)), ((), ())), preferred_element_type=F32)
    image = []
    for tile in range(leg_ref.shape[1] // LANES):
        cols = slice(tile * LANES, (tile + 1) * LANES)
        image.append(vec_refs[0, :, cols] + jnp.where(triangle_tile(wave, tile), adjoint[:, cols], 0.0))
    return image


def scalar_row(value):
    return jnp.broadcast_to(value, (1, LANES))


def middle_kernel(stage, slots, chunk_rows, *refs):
    waves_ref, home_ref, leg_ref, sum_a, sum_b, sum_c, sum_d, past_ref, *refs = refs
    if stage == 0:
        res_ref, new_ref, along_ref, out_ref, norm_ref, hist_ref, acc_ref, held_ref = refs
    else:
        res_ref, last_ref, new_ref, along_ref, out_ref, norm_ref, hist_ref, acc_ref, held_ref = refs
    slot = pl.program_id(0)
    wave = waves_ref[slot]

    @pl.when(slot == 0)
    def _():
        held_ref[...] = home_ref[...].astype(F32)
        norm, product = sums_of((sum_a, sum_b, sum_c, sum_d), chunk_rows)
        hist_ref[...] = jnp.zeros_like(hist_ref)
        if stage == 0:
            alpha = norm / product
            beta = jnp.zeros_like(norm)
            hist_ref[2:3, :] = scalar_row(alpha)
        else:
            beta = norm / past_ref[0:1, 0:1]
            alpha = norm / (product - beta * norm / past_ref[1:2, 0:1])
            hist_ref[2:3, :] = past_ref[2:3, :]
            hist_ref[3:4, :] = scalar_row(alpha)
        hist_ref[0:1, :] = scalar_row(norm)
        hist_ref[1:2, :] = scalar_row(alpha)
        hist_ref[4:5, :] = scalar_row(beta)
        norm_ref[...] = jnp.zeros_like(norm_ref)

    alpha = hist_ref[1:2, :]
    beta = hist_ref[4:5, :]
    image = image_of(res_ref, held_ref, leg_ref, wave, slot, slots, chunk_rows)
    parts = []
    for tile, along in enumerate(image):
        cols = slice(tile * LANES, (tile + 1) * LANES)
        if stage > 0:
            along = along + beta * last_ref[0, :, cols]
        along_ref[0, :, cols] = along
        part = res_ref[0, :, cols] - alpha * along
        new_ref[0, :, cols] = part
        parts.append(part)
    norm_ref[...] += square_sum(parts)
    forward(jnp.concatenate(parts, axis=1), leg_ref, acc_ref, out_ref, slot, slots, chunk_rows)


def last_kernel(slots, chunk_rows, *refs):
    waves_ref, home_ref, leg_ref, sum_a, sum_b, sum_c, sum_d, past_ref, *refs = refs
    res0_ref, res1_ref, res2_ref, last_ref, sol_ref, fin_ref, hist_ref, held_ref = refs
    slot = pl.program_id(0)
    wave = waves_ref[slot]

    @pl.when(slot == 0)
    def _():
        held_ref[...] = home_ref[...].astype(F32)
        norm, product = sums_of((sum_a, sum_b, sum_c, sum_d), chunk_rows)
        beta = norm / past_ref[0:1, 0:1]
        alpha = norm / (product - beta * norm / past_ref[1:2, 0:1])
        hist_ref[0:1, :] = scalar_row(alpha)
        hist_ref[1:2, :] = scalar_row(beta)

    alpha = hist_ref[0:1, :]
    beta = hist_ref[1:2, :]
    alpha0, alpha1, beta1 = past_ref[2:3, :], past_ref[3:4, :], past_ref[4:5, :]
    image = image_of(res2_ref, held_ref, leg_ref, wave, slot, slots, chunk_rows)
    for tile, along in enumerate(image):
        cols = slice(tile * LANES, (tile + 1) * LANES)
        along = along + beta * last_ref[0, :, cols]
        res2 = res2_ref[0, :, cols]
        fin_ref[0, :, cols] = res2 - alpha * along
        first = res0_ref[0, :, cols]
        second = res1_ref[0, :, cols] + beta1 * first
        third = res2 + beta * second
        sol_ref[0, :, cols] = alpha0 * first + alpha1 * second + alpha * third


def fourier_kernel(chunk_rows, slots, norm_factor, lon_count, waves_ref, out_ref):
    rows = waves_ref.shape[0]
    wave = waves_ref[...].astype(F32)
    lane = lax.broadcasted_iota(jnp.int32, (rows, LANES), 1).astype(F32)
    row = lax.broadcasted_iota(jnp.int32, (rows, LANES), 0) + pl.program_id(0) * rows
    within = row - (row // chunk_rows) * chunk_rows
    quarter = jnp.where(within >= slots, 0.25 * lon_count, 0.0)
    fine_cos, fine_sin = turn(wave * lane, lon_count)
    coarse_cos, coarse_sin = turn(wave * (lane * LANES) + quarter, lon_count)
    coarse_cos = coarse_cos * norm_factor
    coarse_sin = coarse_sin * norm_factor
    for tile in range(lon_count // LANES):
        value = coarse_cos[:, tile : tile + 1] * fine_cos - coarse_sin[:, tile : tile + 1] * fine_sin
        out_ref[:, tile * LANES : (tile + 1) * LANES] = value.astype(BF16)


def turn(phase, period):
    phase = phase - period * jnp.floor(phase * (1.0 / period) + 0.5)
    quadrant = jnp.floor(phase * (4.0 / period) + 0.5)
    angle = (phase - quadrant * (0.25 * period)) * (2.0 * math.pi / period)
    sq = angle * angle
    cosine = 1.0 + sq * (-1.0 / 2 + sq * (1.0 / 24 + sq * (-1.0 / 720 + sq * (1.0 / 40320))))
    sine = angle * (1.0 + sq * (-1.0 / 6 + sq * (1.0 / 120 + sq * (-1.0 / 5040 + sq * (1.0 / 362880)))))
    odd = jnp.abs(quadrant) == 1.0
    cos_base = jnp.where(odd, -quadrant * sine, cosine)
    sin_base = jnp.where(odd, quadrant * cosine, sine)
    back = jnp.abs(quadrant) == 2.0
    return jnp.where(back, -cos_base, cos_base), jnp.where(back, -sin_base, sin_base)


def pieces_of(value):
    high = value.astype(BF16).astype(F32)
    middle = (value - high).astype(BF16).astype(F32)
    low = (value - high - middle).astype(BF16).astype(F32)
    return high, middle, low


def grid_kernel(x_ref, table_ref, weight_ref, norm_ref, out_ref, turned_ref, wide_ref):
    count, lons = table_ref.shape
    step = 256
    turned_ref[...] = x_ref[...].astype(F32).T.astype(BF16)
    energy = jnp.zeros((SUB, step), F32)
    for first in range(0, lons, step):
        cols = slice(first, first + step)
        grid = jnp.dot(turned_ref[...], table_ref[:, cols], preferred_element_type=F32)
        weight = weight_ref[:, cols]
        weighted = []
        for group in range(GROUPS):
            rows = grid[group * PIECE : (group + 1) * PIECE]
            product = weight * rows
            weighted.append(product)
            square = product * rows
            for block in range(0, PIECE, SUB):
                energy = energy + square[block : block + SUB]
        weighted.append(jnp.zeros((LANES - SPARE, step), F32))
        wide_ref[cols, :] = jnp.concatenate(weighted, axis=0).T.astype(BF16)
    lane = lane_of(1)
    spare = jnp.zeros((1, LANES), F32)
    values = pieces_of(jnp.sum(norm_ref[...], axis=(0, 1), keepdims=True))
    values = values + pieces_of(jnp.sum(energy, axis=(0, 1), keepdims=True))
    for place, value in enumerate(values):
        spare = jnp.where(lane == SPARE + place, value, spare)
    for first in range(0, count, step):
        rows = slice(first, first + step)
        back = jnp.dot(table_ref[rows, :], wide_ref[...], preferred_element_type=F32)
        out_ref[rows, :] = jnp.where(lane >= SPARE, spare, back).astype(BF16)


def tail_kernel(x_ref, out_ref):
    total = jnp.zeros((SUB, LANES), F32)
    block = 2 * SUB
    for first in range(0, x_ref.shape[0], block):
        value = x_ref[first : first + block, :].astype(F32)
        total = total + value[:SUB] + value[SUB:]
    out_ref[...] = total


def exchange(payload, parts):
    rows = payload.shape[0]
    packed = payload.reshape(parts, rows // parts // 2, 2, LANES)
    return lax.all_to_all(packed, EXCHANGE, 0, 0, tiled=True).reshape(rows, LANES)


def whole(shape):
    return pl.BlockSpec(shape, lambda *_: (0,) * len(shape))


def on_device(right_side, legendre, wave_map, obs_weight):
    slots, degrees, lats = legendre.shape
    lon_count = obs_weight.shape[1]
    bands = ZS * YS * CS
    rows = bands * 2 * slots
    chunk_rows = 2 * slots
    band_at = lax.axis_index(BAND)
    own_waves = lax.dynamic_slice_in_dim(wave_map, band_at * slots, slots)

    vec = right_side.reshape(slots, 2, GROUPS, YS, degrees).transpose(0, 2, 3, 1, 4)
    vec = vec.reshape(slots, GROUPS * SUB, degrees)

    spread = wave_map.reshape(ZS, YS, CS, slots).transpose(0, 2, 1, 3).reshape(bands, 1, slots)
    spread = jnp.broadcast_to(spread, (bands, 2, slots)).reshape(rows, 1)
    spread = jnp.broadcast_to(spread, (rows, LANES))
    block = 128
    table = pl.pallas_call(
        functools.partial(fourier_kernel, chunk_rows, slots, 1.0 / math.sqrt(wave_map.shape[0]), lon_count),
        grid=(rows // block,),
        in_specs=[pl.BlockSpec((block, LANES), lambda i: (i, 0))],
        out_specs=pl.BlockSpec((block, lon_count), lambda i: (i, 0)),
        out_shape=jax.ShapeDtypeStruct((rows, lon_count), BF16),
        cost_estimate=pl.CostEstimate(flops=4_000_000_000, bytes_accessed=4_000_000, transcendentals=0),
        compiler_params=pltpu.CompilerParams(vmem_limit_bytes=16 * 1024 * 1024),
        name="fourier",
    )(spread)

    near = jnp.broadcast_to(obs_weight[None], (YS * CS,) + obs_weight.shape)
    near = lax.all_to_all(near, ("y", "c"), 0, 0, tiled=True)
    near = lax.dynamic_slice_in_dim(near, lax.axis_index("c") * YS, YS)
    weight = near.reshape(PIECE, lon_count)

    slot_block = pl.BlockSpec((1, GROUPS * SUB, degrees), lambda i: (i, 0, 0))
    leg_block = pl.BlockSpec((1, degrees, lats), lambda i: (i, 0, 0))
    smem = pl.BlockSpec(memory_space=pltpu.SMEM)
    small = whole((SUB, LANES))
    payload_block = whole((rows, LANES))
    vec_shape = jax.ShapeDtypeStruct((slots, GROUPS * SUB, degrees), F32)
    payload_shape = jax.ShapeDtypeStruct((rows, LANES), BF16)
    small_shape = jax.ShapeDtypeStruct((SUB, LANES), F32)
    held = pltpu.VMEM((rows, LANES), F32)
    cost = pl.CostEstimate(flops=4_000_000_000, bytes_accessed=9_000_000, transcendentals=0)

    res, payload, norm = pl.pallas_call(
        functools.partial(first_kernel, slots, chunk_rows),
        grid=(slots,),
        in_specs=[smem, slot_block, leg_block],
        out_specs=[slot_block, payload_block, small],
        out_shape=[vec_shape, payload_shape, small_shape],
        scratch_shapes=[held],
        cost_estimate=cost,
        compiler_params=pltpu.CompilerParams(vmem_limit_bytes=16 * 1024 * 1024),
        name="first",
    )(own_waves, vec, legendre)

    def reach(payload, norm):
        arrived = exchange(payload, bands)
        back = pl.pallas_call(
            grid_kernel,
            out_shape=payload_shape,
            scratch_shapes=[pltpu.VMEM((LANES, rows), BF16), pltpu.VMEM((lon_count, LANES), BF16)],
            cost_estimate=cost,
            compiler_params=pltpu.CompilerParams(vmem_limit_bytes=16 * 1024 * 1024),
        name="grid",
        )(arrived, table, weight, norm)
        home = exchange(back, bands)
        sums = pl.pallas_call(
            tail_kernel,
            out_shape=small_shape,
            compiler_params=pltpu.CompilerParams(vmem_limit_bytes=16 * 1024 * 1024),
        name="tail",
        )(home)
        others = [lax.ppermute(sums, "x", [(i, (i + k) % XS) for i in range(XS)]) for k in range(1, XS)]
        return home, [sums] + others

    past = jnp.zeros((SUB, LANES), F32)
    residuals = [res]
    along = None
    for stage in range(2):
        home, sums = reach(payload, norm)
        operands = [own_waves, home, legendre, *sums, past, residuals[-1]]
        specs = [smem, payload_block, leg_block, small, small, small, small, small, slot_block]
        if stage > 0:
            operands.append(along)
            specs.append(slot_block)
        res, along, payload, norm, past = pl.pallas_call(
            functools.partial(middle_kernel, stage, slots, chunk_rows),
            grid=(slots,),
            in_specs=specs,
            out_specs=[slot_block, slot_block, payload_block, small, small],
            out_shape=[vec_shape, vec_shape, payload_shape, small_shape, small_shape],
            scratch_shapes=[held, held],
            cost_estimate=cost,
            compiler_params=pltpu.CompilerParams(vmem_limit_bytes=16 * 1024 * 1024),
            name=f"middle{stage}",
        )(*operands)
        residuals.append(res)
    home, sums = reach(payload, norm)
    solution, residual = pl.pallas_call(
        functools.partial(last_kernel, slots, chunk_rows),
        grid=(slots,),
        in_specs=[smem, payload_block, leg_block, small, small, small, small, small] + [slot_block] * 4,
        out_specs=[slot_block, slot_block],
        out_shape=[vec_shape, vec_shape],
        scratch_shapes=[pltpu.VMEM((SUB, LANES), F32), held],
        cost_estimate=cost,
        compiler_params=pltpu.CompilerParams(vmem_limit_bytes=16 * 1024 * 1024),
        name="last",
    )(own_waves, home, legendre, *sums, past, *residuals, along)

    def unpack(value):
        value = value.reshape(slots, GROUPS, YS, 2, degrees).transpose(0, 3, 1, 2, 4)
        return value.reshape(right_side.shape)

    return unpack(solution), unpack(residual)


def solution(mesh):
    split = Mesh(mesh.devices.reshape(ZS, YS, CS, XS), ("z", "y", "c", "x"))
    return jax.shard_map(
        on_device,
        mesh=split,
        in_specs=(P(BAND, None, "x", None, None), P(BAND, None, None), P(), P(BAND, None)),
        out_specs=(P(BAND, None, "x", None, None), P(BAND, None, "x", None, None)),
        check_vma=False,
    )
```

```python
import functools
import math

import jax
import jax.numpy as jnp
from jax import lax
from jax.experimental import pallas as pl
from jax.experimental.pallas import tpu as pltpu
from jax.sharding import Mesh
from jax.sharding import PartitionSpec as P

ZS, YS, CS, XS = 8, 4, 2, 4
BAND = ("z", "y", "c")
GROUPS = 3
SHARES = 4
PIECE = 40
PIECES = 16
SUB = 8
LANES = 128
SPARE = GROUPS * PIECE
F32 = jnp.float32
BF16 = jnp.bfloat16
UNROLL = 2


def lane_of(rows=SUB):
    return lax.broadcasted_iota(jnp.int32, (rows, LANES), 1)


def scatter_rows(value, acc_ref, slot, chunk_rows, slots):
    lane = lane_of()
    for piece in range(PIECES):
        first = piece * PIECE
        tile, offset = first // LANES, first % LANES
        out = jnp.zeros((SUB, LANES), F32)
        for group in reversed(range(GROUPS)):
            rows = slice(group * SUB, (group + 1) * SUB)
            source = value[rows, tile * LANES : (tile + 1) * LANES]
            if offset + PIECE > LANES:
                following = value[rows, (tile + 1) * LANES : (tile + 2) * LANES]
                source = jnp.where(lane >= offset, source, following)
            shift = (group * PIECE - offset) % LANES
            if shift:
                source = pltpu.roll(source, shift, 1)
            out = jnp.where(lane < (group + 1) * PIECE, source, out)
        acc_ref[pl.ds(piece * SHARES * chunk_rows + slot, SUB, stride=slots), :] = out


def gather_rows(held_ref, slot, chunk_rows, slots, lat_tiles):
    lane = lane_of()
    tiles = [[None] * lat_tiles for _ in range(GROUPS)]
    for piece in range(PIECES):
        first = piece * PIECE
        tile, offset = first // LANES, first % LANES
        rows = held_ref[pl.ds(piece * SHARES * chunk_rows + slot, SUB, stride=slots), :]
        for group in range(GROUPS):
            shift = (offset - group * PIECE) % LANES
            moved = pltpu.roll(rows, shift, 1) if shift else rows
            known = tiles[group][tile]
            tiles[group][tile] = moved if known is None else jnp.where(lane >= offset, moved, known)
            if offset + PIECE > LANES:
                tiles[group][tile + 1] = moved
    return jnp.concatenate([jnp.concatenate(row, axis=1) for row in tiles], axis=0)


def square_sum(parts):
    total = None
    for part in parts:
        for group in range(GROUPS):
            block = part[group * SUB : (group + 1) * SUB, :]
            total = block * block if total is None else total + block * block
    return total


def triangle_tile(wave, tile):
    return lane_of(GROUPS * SUB) + tile * LANES >= wave


def band_index():
    return (lax.axis_index("z") * YS + lax.axis_index("y")) * CS + lax.axis_index("c")


def wave_of(waves_ref, slots, slot):
    return waves_ref[band_index() * slots + slot]


def flat_rows(slot, group, tile, part, tiles):
    first = ((slot * 2 + part) * GROUPS + group) * SHARES * tiles + tile
    return pl.ds(first, SHARES, stride=tiles)


def first_kernel(slots, chunk_rows, waves_ref, vec_ref, leg_ref, res_ref, out_ref, norm_ref, acc_ref, turn_ref):
    tiles = leg_ref.shape[1] // LANES
    norm_ref[...] = jnp.zeros_like(norm_ref)

    def step(slot, carry):
        wave = wave_of(waves_ref, slots, slot)
        parts = []
        for tile in range(tiles):
            cols = slice(tile * LANES, (tile + 1) * LANES)
            for group in range(GROUPS):
                for part in range(2):
                    rows = vec_ref[flat_rows(slot, group, tile, part, tiles), :]
                    turn_ref[pl.ds(group * SUB + part, SHARES, stride=2), :] = rows
            parts.append(jnp.where(triangle_tile(wave, tile), turn_ref[...], 0.0))
            res_ref[slot, :, cols] = parts[-1]
        norm_ref[...] += square_sum(parts)
        forward(jnp.concatenate(parts, axis=1), leg_ref, acc_ref, slot, slots, chunk_rows)
        return carry

    lax.fori_loop(0, slots, step, 0, unroll=UNROLL)
    out_ref[...] = acc_ref[...].astype(BF16)


def forward(vector, leg_ref, acc_ref, slot, slots, chunk_rows):
    coeffs = jnp.dot(vector.astype(BF16), leg_ref[slot], preferred_element_type=F32)
    scatter_rows(coeffs, acc_ref, slot, chunk_rows, slots)


def sums_of(sum_refs, chunk_rows):
    total = sum_refs[0][...]
    for ref in sum_refs[1:]:
        total = total + ref[...]
    total = total * (1.0 / chunk_rows)
    lane = lane_of()
    norm = jnp.sum(jnp.where((lane >= SPARE) & (lane < SPARE + 3), total, 0.0), axis=(0, 1), keepdims=True)
    energy = jnp.sum(jnp.where((lane >= SPARE + 3) & (lane < SPARE + 6), total, 0.0), axis=(0, 1), keepdims=True)
    return norm, norm + energy


def back_kernel(slots, chunk_rows, waves_ref, home_ref, leg_ref, adj_ref, held_ref):
    held_ref[...] = home_ref[...].astype(F32)
    tiles = leg_ref.shape[2] // LANES

    def step(slot, carry):
        wave = wave_of(waves_ref, slots, slot)
        home = gather_rows(held_ref, slot, chunk_rows, slots, tiles).astype(BF16)
        adjoint = lax.dot_general(home, leg_ref[slot], (((1,), (1,)), ((), ())), preferred_element_type=F32)
        for tile in range(leg_ref.shape[1] // LANES):
            cols = slice(tile * LANES, (tile + 1) * LANES)
            adj_ref[slot, :, cols] = jnp.where(triangle_tile(wave, tile), adjoint[:, cols], 0.0)
        return carry

    lax.fori_loop(0, slots, step, 0, unroll=UNROLL)


def scalar_row(value):
    return jnp.broadcast_to(value, (1, LANES))


def middle_kernel(stage, slots, chunk_rows, *refs):
    if stage == 0:
        sum_a, sum_b, sum_c, sum_d, leg_ref, adj_ref, res_ref, *refs = refs
    else:
        sum_a, sum_b, sum_c, sum_d, leg_ref, adj_ref, res_ref, last_ref, past_ref, *refs = refs
    new_ref, along_ref, out_ref, norm_ref, hist_ref, acc_ref = refs
    norm, product = sums_of((sum_a, sum_b, sum_c, sum_d), chunk_rows)
    hist_ref[...] = jnp.zeros_like(hist_ref)
    if stage == 0:
        alpha = norm / product
        beta = jnp.zeros_like(norm)
        hist_ref[2:3, :] = scalar_row(alpha)
    else:
        beta = norm / past_ref[0:1, 0:1]
        alpha = norm / (product - beta * norm / past_ref[1:2, 0:1])
        hist_ref[2:3, :] = past_ref[2:3, :]
        hist_ref[3:4, :] = scalar_row(alpha)
    hist_ref[0:1, :] = scalar_row(norm)
    hist_ref[1:2, :] = scalar_row(alpha)
    hist_ref[4:5, :] = scalar_row(beta)
    norm_ref[...] = jnp.zeros_like(norm_ref)

    def step(slot, carry):
        alpha = hist_ref[1:2, :]
        beta = hist_ref[4:5, :]
        parts = []
        for tile in range(leg_ref.shape[1] // LANES):
            cols = slice(tile * LANES, (tile + 1) * LANES)
            res = res_ref[slot, :, cols]
            along = res + adj_ref[slot, :, cols]
            if stage > 0:
                along = along + beta * last_ref[slot, :, cols]
            along_ref[slot, :, cols] = along
            part = res - alpha * along
            new_ref[slot, :, cols] = part
            parts.append(part)
        norm_ref[...] += square_sum(parts)
        forward(jnp.concatenate(parts, axis=1), leg_ref, acc_ref, slot, slots, chunk_rows)
        return carry

    lax.fori_loop(0, slots, step, 0, unroll=UNROLL)
    out_ref[...] = acc_ref[...].astype(BF16)


def last_kernel(slots, chunk_rows, *refs):
    sum_a, sum_b, sum_c, sum_d, adj_ref, res0_ref, res1_ref, res2_ref, last_ref, past_ref, *refs = refs
    sol_ref, fin_ref, turn_ref = refs
    norm, product = sums_of((sum_a, sum_b, sum_c, sum_d), chunk_rows)
    beta = norm / past_ref[0:1, 0:1]
    alpha = scalar_row(norm / (product - beta * norm / past_ref[1:2, 0:1]))
    beta = scalar_row(beta)
    alpha0, alpha1, beta1 = past_ref[2:3, :], past_ref[3:4, :], past_ref[4:5, :]
    tiles = adj_ref.shape[2] // LANES
    height = GROUPS * SUB

    def step(slot, carry):
        for tile in range(tiles):
            cols = slice(tile * LANES, (tile + 1) * LANES)
            res2 = res2_ref[slot, :, cols]
            along = res2 + adj_ref[slot, :, cols] + beta * last_ref[slot, :, cols]
            first = res0_ref[slot, :, cols]
            second = res1_ref[slot, :, cols] + beta1 * first
            third = res2 + beta * second
            turn_ref[(2 * tile) * height : (2 * tile + 1) * height, :] = res2 - alpha * along
            turn_ref[(2 * tile + 1) * height : (2 * tile + 2) * height, :] = (
                alpha0 * first + alpha1 * second + alpha * third
            )
            for group in range(GROUPS):
                for part in range(2):
                    rows = flat_rows(slot, group, tile, part, tiles)
                    at = group * SUB + part
                    fin_ref[rows, :] = turn_ref[pl.ds((2 * tile) * height + at, SHARES, stride=2), :]
                    sol_ref[rows, :] = turn_ref[pl.ds((2 * tile + 1) * height + at, SHARES, stride=2), :]
        return carry

    lax.fori_loop(0, slots, step, 0)


def fourier_kernel(chunk_rows, slots, norm_factor, waves_ref, out_ref):
    rows = 32
    lon_count = out_ref.shape[1]
    lane = lax.broadcasted_iota(jnp.int32, (rows, LANES), 1).astype(F32)
    local = lax.broadcasted_iota(jnp.int32, (rows, LANES), 0)

    def step(index, carry):
        at = pl.multiple_of(index * rows, rows)
        wave = waves_ref[pl.ds(at, rows), :].astype(F32)
        row = (local + at).astype(F32)
        within = row - chunk_rows * jnp.floor((row + 0.5) * (1.0 / chunk_rows))
        quarter = jnp.where(within > slots - 0.5, 0.25 * lon_count, 0.0)
        cosine, sine = turn(wave * lane + quarter, lon_count)
        cosine = cosine * norm_factor
        sine = sine * norm_factor
        step_cos, step_sin = turn(wave * float(LANES), lon_count)
        for tile in range(lon_count // LANES):
            out_ref[pl.ds(at, rows), tile * LANES : (tile + 1) * LANES] = cosine.astype(BF16)
            cosine, sine = cosine * step_cos - sine * step_sin, sine * step_cos + cosine * step_sin
        return carry

    lax.fori_loop(0, waves_ref.shape[0] // rows, step, 0)


def weight_kernel(*refs):
    *near_refs, out_ref, held_ref = refs
    height = near_refs[0].shape[0]
    for turn_at, near_ref in enumerate(near_refs):
        held_ref[turn_at, :height, :] = near_ref[...]
    share = lax.rem(band_index(), SHARES)
    for place in range(SHARES):
        out_ref[place * height : (place + 1) * height, :] = held_ref[jnp.bitwise_xor(share, place), :height, :]


def turn(phase, period):
    phase = phase - period * jnp.floor(phase * (1.0 / period) + 0.5)
    quadrant = jnp.floor(phase * (4.0 / period) + 0.5)
    angle = (phase - quadrant * (0.25 * period)) * (2.0 * math.pi / period)
    sq = angle * angle
    cosine = 1.0 + sq * (-1.0 / 2 + sq * (1.0 / 24 + sq * (-1.0 / 720 + sq * (1.0 / 40320))))
    sine = angle * (1.0 + sq * (-1.0 / 6 + sq * (1.0 / 120 + sq * (-1.0 / 5040 + sq * (1.0 / 362880)))))
    odd = jnp.abs(quadrant) == 1.0
    cos_base = jnp.where(odd, -quadrant * sine, cosine)
    sin_base = jnp.where(odd, quadrant * cosine, sine)
    back = jnp.abs(quadrant) == 2.0
    return jnp.where(back, -cos_base, cos_base), jnp.where(back, -sin_base, sin_base)


def pieces_of(value):
    high = value.astype(BF16).astype(F32)
    middle = (value - high).astype(BF16).astype(F32)
    low = (value - high - middle).astype(BF16).astype(F32)
    return high, middle, low


def grid_kernel(x_ref, table_ref, weight_ref, norm_ref, out_ref, turned_ref, wide_ref):
    count, lons = table_ref.shape
    step = 256
    turned_ref[...] = x_ref[...].astype(F32).T.astype(BF16)
    energy = jnp.zeros((SUB, step), F32)
    for first in range(0, lons, step):
        cols = slice(first, first + step)
        grid = jnp.dot(turned_ref[...], table_ref[:, cols], preferred_element_type=F32)
        weight = weight_ref[:, cols]
        weighted = []
        for group in range(GROUPS):
            rows = grid[group * PIECE : (group + 1) * PIECE]
            product = weight * rows
            weighted.append(product)
            square = product * rows
            for block in range(0, PIECE, SUB):
                energy = energy + square[block : block + SUB]
        weighted.append(jnp.zeros((LANES - SPARE, step), F32))
        wide_ref[cols, :] = jnp.concatenate(weighted, axis=0).T.astype(BF16)
    lane = lane_of(1)
    spare = jnp.zeros((1, LANES), F32)
    values = pieces_of(jnp.sum(norm_ref[...], axis=(0, 1), keepdims=True))
    values = values + pieces_of(jnp.sum(energy, axis=(0, 1), keepdims=True))
    for place, value in enumerate(values):
        spare = jnp.where(lane == SPARE + place, value, spare)
    for first in range(0, count, step):
        rows = slice(first, first + step)
        back = jnp.dot(table_ref[rows, :], wide_ref[...], preferred_element_type=F32)
        out_ref[rows, :] = jnp.where(lane >= SPARE, spare, back).astype(BF16)


def tail_kernel(x_ref, out_ref):
    total = jnp.zeros((SUB, LANES), F32)
    block = 2 * SUB
    for first in range(0, x_ref.shape[0], block):
        value = x_ref[first : first + block, :].astype(F32)
        total = total + value[:SUB] + value[SUB:]
    out_ref[...] = total


def exchange(payload, parts):
    rows = payload.shape[0]
    packed = payload.reshape(parts, rows // parts // 2, 2, LANES)
    return lax.all_to_all(packed, BAND, 0, 0, tiled=True).reshape(rows, LANES)


def call(kernel, name, outs, ins, scratch=(), vmem=24, flops=2_000_000_000):
    return pl.pallas_call(
        kernel,
        in_specs=ins,
        out_specs=[pl.BlockSpec(memory_space=pltpu.VMEM)] * len(outs),
        out_shape=outs,
        scratch_shapes=scratch,
        compiler_params=pltpu.CompilerParams(vmem_limit_bytes=vmem * 1024 * 1024),
        cost_estimate=pl.CostEstimate(flops=flops, bytes_accessed=1_000_000, transcendentals=0),
        name=name,
    )


def on_device(right_side, legendre, wave_map, obs_weight):
    slots, degrees, lats = legendre.shape
    lon_count = obs_weight.shape[1]
    bands = ZS * YS * CS
    rows = bands * 2 * slots
    chunk_rows = 2 * slots
    smem = pl.BlockSpec(memory_space=pltpu.SMEM)
    vmem = pl.BlockSpec(memory_space=pltpu.VMEM)
    flat = right_side.reshape(-1, LANES)
    spread = jnp.broadcast_to(wave_map.reshape(bands, 1, slots), (bands, 2, slots)).reshape(rows, 1)
    spread = jnp.broadcast_to(spread, (rows, LANES))
    flat, spread = lax.optimization_barrier((flat, spread))

    vec_shape = jax.ShapeDtypeStruct((slots, GROUPS * SUB, degrees), F32)
    payload_shape = jax.ShapeDtypeStruct((rows, LANES), BF16)
    small_shape = jax.ShapeDtypeStruct((SUB, LANES), F32)
    flat_shape = jax.ShapeDtypeStruct(flat.shape, F32)
    held = pltpu.VMEM((rows, LANES), F32)

    (table,) = call(
        functools.partial(fourier_kernel, chunk_rows, slots, 1.0 / math.sqrt(wave_map.shape[0])),
        "fourier",
        [jax.ShapeDtypeStruct((rows, lon_count), BF16)],
        [vmem],
        flops=4_000_000_000,
    )(spread)
    flat, table = lax.optimization_barrier((flat, table))

    res, payload, norm = call(
        functools.partial(first_kernel, slots, chunk_rows),
        "first",
        [vec_shape, payload_shape, small_shape],
        [smem, vmem, vmem],
        [held, pltpu.VMEM((GROUPS * SUB, LANES), F32)],
    )(wave_map, flat, legendre)

    near = [obs_weight]
    for turn_at in range(1, SHARES):
        pairs = [(at, at ^ turn_at) for at in range(YS * CS)]
        near.append(lax.ppermute(obs_weight, ("y", "c"), pairs))
    (weight,) = call(
        weight_kernel,
        "weight",
        [jax.ShapeDtypeStruct((PIECE, lon_count), F32)],
        [vmem] * SHARES,
        [pltpu.VMEM((SHARES, 2 * SUB, lon_count), F32)],
    )(*near)
    payload, table, weight = lax.optimization_barrier((payload, table, weight))

    def reach(payload, norm):
        arrived = exchange(payload, bands)
        (back,) = call(
            grid_kernel,
            "grid",
            [payload_shape],
            [vmem] * 4,
            [pltpu.VMEM((LANES, rows), BF16), pltpu.VMEM((lon_count, LANES), BF16)],
        )(arrived, table, weight, norm)
        home = exchange(back, bands)
        (sums,) = call(tail_kernel, "tail", [small_shape], [vmem])(home)
        others = [lax.ppermute(sums, "x", [(i, (i + k) % XS) for i in range(XS)]) for k in range(1, XS)]
        (adjoint,) = call(
            functools.partial(back_kernel, slots, chunk_rows),
            "back",
            [vec_shape],
            [smem, vmem, vmem],
            [held],
            flops=8_000_000_000,
        )(wave_map, home, legendre)
        return adjoint, [sums] + others

    residuals = [res]
    carried = []
    for stage in range(2):
        adjoint, sums = reach(payload, norm)
        operands = [*sums, legendre, adjoint, residuals[-1], *carried]
        res, along, payload, norm, past = call(
            functools.partial(middle_kernel, stage, slots, chunk_rows),
            f"middle{stage}",
            [vec_shape, vec_shape, payload_shape, small_shape, small_shape],
            [vmem] * len(operands),
            [held],
        )(*operands)
        residuals.append(res)
        carried = [along, past]
    adjoint, sums = reach(payload, norm)
    solution, residual = call(
        functools.partial(last_kernel, slots, chunk_rows),
        "last",
        [flat_shape, flat_shape],
        [vmem] * 10,
        [pltpu.VMEM((2 * GROUPS * SUB * (degrees // LANES), LANES), F32)],
    )(*sums, adjoint, *residuals, along, past)
    return solution.reshape(right_side.shape), residual.reshape(right_side.shape)


def solution(mesh):
    split = Mesh(mesh.devices.reshape(ZS, YS, CS, XS), ("z", "y", "c", "x"))
    return jax.shard_map(
        on_device,
        mesh=split,
        in_specs=(P(BAND, None, "x", None, None), P(BAND, None, None), P(), P(BAND, None)),
        out_specs=(P(BAND, None, "x", None, None), P(BAND, None, "x", None, None)),
        check_vma=False,
    )
```

```python
import functools
import math

import jax
import jax.numpy as jnp
from jax import lax
from jax.experimental import pallas as pl
from jax.experimental.pallas import tpu as pltpu
from jax.sharding import Mesh
from jax.sharding import PartitionSpec as P

ZS, YS, CS, XS = 8, 4, 2, 4
BAND = ("z", "y", "c")
GROUPS = 3
SHARES = 4
PIECE = 40
PIECES = 16
SUB = 8
LANES = 128
SPARE = GROUPS * PIECE
F32 = jnp.float32
BF16 = jnp.bfloat16
UNROLL = 10


def lane_of(rows=SUB):
    return lax.broadcasted_iota(jnp.int32, (rows, LANES), 1)


def scatter_rows(value, acc_ref, slot, chunk_rows, slots):
    lane = lane_of()
    for piece in range(PIECES):
        first = piece * PIECE
        tile, offset = first // LANES, first % LANES
        out = jnp.zeros((SUB, LANES), F32)
        for group in reversed(range(GROUPS)):
            rows = slice(group * SUB, (group + 1) * SUB)
            source = value[rows, tile * LANES : (tile + 1) * LANES]
            if offset + PIECE > LANES:
                following = value[rows, (tile + 1) * LANES : (tile + 2) * LANES]
                source = jnp.where(lane >= offset, source, following)
            shift = (group * PIECE - offset) % LANES
            if shift:
                source = pltpu.roll(source, shift, 1)
            out = jnp.where(lane < (group + 1) * PIECE, source, out)
        acc_ref[pl.ds(piece * SHARES * chunk_rows + slot, SUB, stride=slots), :] = out


def gather_rows(held_ref, slot, chunk_rows, slots, lat_tiles):
    lane = lane_of()
    tiles = [[None] * lat_tiles for _ in range(GROUPS)]
    for piece in range(PIECES):
        first = piece * PIECE
        tile, offset = first // LANES, first % LANES
        rows = held_ref[pl.ds(piece * SHARES * chunk_rows + slot, SUB, stride=slots), :]
        for group in range(GROUPS):
            shift = (offset - group * PIECE) % LANES
            moved = pltpu.roll(rows, shift, 1) if shift else rows
            known = tiles[group][tile]
            tiles[group][tile] = moved if known is None else jnp.where(lane >= offset, moved, known)
            if offset + PIECE > LANES:
                tiles[group][tile + 1] = moved
    return jnp.concatenate([jnp.concatenate(row, axis=1) for row in tiles], axis=0)


def square_sum(parts):
    total = None
    for part in parts:
        for group in range(GROUPS):
            block = part[group * SUB : (group + 1) * SUB, :]
            total = block * block if total is None else total + block * block
    return total


def triangle_tile(wave, tile):
    return lane_of(GROUPS * SUB) + tile * LANES >= wave


def band_index():
    return (lax.axis_index("z") * YS + lax.axis_index("y")) * CS + lax.axis_index("c")


def wave_of(waves_ref, slots, slot):
    return waves_ref[band_index() * slots + slot]


def flat_rows(slot, group, tile, part, tiles):
    first = ((slot * 2 + part) * GROUPS + group) * SHARES * tiles + tile
    return pl.ds(first, SHARES, stride=tiles)


def first_kernel(slots, chunk_rows, waves_ref, vec_ref, leg_ref, res_ref, out_ref, norm_ref, acc_ref, turn_ref):
    tiles = leg_ref.shape[1] // LANES
    norm_ref[...] = jnp.zeros_like(norm_ref)

    def step(slot, carry):
        wave = wave_of(waves_ref, slots, slot)
        parts = []
        for tile in range(tiles):
            cols = slice(tile * LANES, (tile + 1) * LANES)
            for group in range(GROUPS):
                for part in range(2):
                    rows = vec_ref[flat_rows(slot, group, tile, part, tiles), :]
                    turn_ref[pl.ds(group * SUB + part, SHARES, stride=2), :] = rows
            parts.append(jnp.where(triangle_tile(wave, tile), turn_ref[...], 0.0))
            res_ref[slot, :, cols] = parts[-1]
        norm_ref[...] += square_sum(parts)
        forward(jnp.concatenate(parts, axis=1), leg_ref, acc_ref, slot, slots, chunk_rows)
        return carry

    lax.fori_loop(0, slots, step, 0, unroll=UNROLL)
    out_ref[...] = acc_ref[...].astype(BF16)


def forward(vector, leg_ref, acc_ref, slot, slots, chunk_rows):
    coeffs = jnp.dot(vector.astype(BF16), leg_ref[slot], preferred_element_type=F32)
    scatter_rows(coeffs, acc_ref, slot, chunk_rows, slots)


def sums_of(sum_refs, chunk_rows):
    total = sum_refs[0][...]
    for ref in sum_refs[1:]:
        total = total + ref[...]
    total = total * (1.0 / chunk_rows)
    lane = lane_of()
    norm = jnp.sum(jnp.where((lane >= SPARE) & (lane < SPARE + 3), total, 0.0), axis=(0, 1), keepdims=True)
    energy = jnp.sum(jnp.where((lane >= SPARE + 3) & (lane < SPARE + 6), total, 0.0), axis=(0, 1), keepdims=True)
    return norm, norm + energy


def back_kernel(slots, chunk_rows, waves_ref, home_ref, leg_ref, adj_ref, held_ref):
    held_ref[...] = home_ref[...].astype(F32)
    tiles = leg_ref.shape[2] // LANES

    def step(slot, carry):
        wave = wave_of(waves_ref, slots, slot)
        home = gather_rows(held_ref, slot, chunk_rows, slots, tiles).astype(BF16)
        adjoint = lax.dot_general(home, leg_ref[slot], (((1,), (1,)), ((), ())), preferred_element_type=F32)
        for tile in range(leg_ref.shape[1] // LANES):
            cols = slice(tile * LANES, (tile + 1) * LANES)
            adj_ref[slot, :, cols] = jnp.where(triangle_tile(wave, tile), adjoint[:, cols], 0.0)
        return carry

    lax.fori_loop(0, slots, step, 0, unroll=UNROLL)


def scalar_row(value):
    return jnp.broadcast_to(value, (1, LANES))


def middle_kernel(stage, slots, chunk_rows, *refs):
    if stage == 0:
        sum_a, sum_b, sum_c, sum_d, leg_ref, adj_ref, res_ref, *refs = refs
    else:
        sum_a, sum_b, sum_c, sum_d, leg_ref, adj_ref, res_ref, last_ref, past_ref, *refs = refs
    new_ref, along_ref, out_ref, norm_ref, hist_ref, acc_ref = refs
    norm, product = sums_of((sum_a, sum_b, sum_c, sum_d), chunk_rows)
    hist_ref[...] = jnp.zeros_like(hist_ref)
    if stage == 0:
        alpha = norm / product
        beta = jnp.zeros_like(norm)
        hist_ref[2:3, :] = scalar_row(alpha)
    else:
        beta = norm / past_ref[0:1, 0:1]
        alpha = norm / (product - beta * norm / past_ref[1:2, 0:1])
        hist_ref[2:3, :] = past_ref[2:3, :]
        hist_ref[3:4, :] = scalar_row(alpha)
    hist_ref[0:1, :] = scalar_row(norm)
    hist_ref[1:2, :] = scalar_row(alpha)
    hist_ref[4:5, :] = scalar_row(beta)
    norm_ref[...] = jnp.zeros_like(norm_ref)

    def step(slot, carry):
        alpha = hist_ref[1:2, :]
        beta = hist_ref[4:5, :]
        parts = []
        for tile in range(leg_ref.shape[1] // LANES):
            cols = slice(tile * LANES, (tile + 1) * LANES)
            res = res_ref[slot, :, cols]
            along = res + adj_ref[slot, :, cols]
            if stage > 0:
                along = along + beta * last_ref[slot, :, cols]
            along_ref[slot, :, cols] = along
            part = res - alpha * along
            new_ref[slot, :, cols] = part
            parts.append(part)
        norm_ref[...] += square_sum(parts)
        forward(jnp.concatenate(parts, axis=1), leg_ref, acc_ref, slot, slots, chunk_rows)
        return carry

    lax.fori_loop(0, slots, step, 0, unroll=UNROLL)
    out_ref[...] = acc_ref[...].astype(BF16)


def last_kernel(slots, chunk_rows, *refs):
    sum_a, sum_b, sum_c, sum_d, adj_ref, res0_ref, res1_ref, res2_ref, last_ref, past_ref, *refs = refs
    sol_ref, fin_ref, turn_ref = refs
    norm, product = sums_of((sum_a, sum_b, sum_c, sum_d), chunk_rows)
    beta = norm / past_ref[0:1, 0:1]
    alpha = scalar_row(norm / (product - beta * norm / past_ref[1:2, 0:1]))
    beta = scalar_row(beta)
    alpha0, alpha1, beta1 = past_ref[2:3, :], past_ref[3:4, :], past_ref[4:5, :]
    tiles = adj_ref.shape[2] // LANES
    height = GROUPS * SUB

    def step(slot, carry):
        for tile in range(tiles):
            cols = slice(tile * LANES, (tile + 1) * LANES)
            res2 = res2_ref[slot, :, cols]
            along = res2 + adj_ref[slot, :, cols] + beta * last_ref[slot, :, cols]
            first = res0_ref[slot, :, cols]
            second = res1_ref[slot, :, cols] + beta1 * first
            third = res2 + beta * second
            turn_ref[(2 * tile) * height : (2 * tile + 1) * height, :] = res2 - alpha * along
            turn_ref[(2 * tile + 1) * height : (2 * tile + 2) * height, :] = (
                alpha0 * first + alpha1 * second + alpha * third
            )
            for group in range(GROUPS):
                for part in range(2):
                    rows = flat_rows(slot, group, tile, part, tiles)
                    at = group * SUB + part
                    fin_ref[rows, :] = turn_ref[pl.ds((2 * tile) * height + at, SHARES, stride=2), :]
                    sol_ref[rows, :] = turn_ref[pl.ds((2 * tile + 1) * height + at, SHARES, stride=2), :]
        return carry

    lax.fori_loop(0, slots, step, 0)


def fourier_kernel(chunk_rows, slots, norm_factor, waves_ref, out_ref):
    rows = 32
    lon_count = out_ref.shape[1]
    lane = lax.broadcasted_iota(jnp.int32, (rows, LANES), 1).astype(F32)
    local = lax.broadcasted_iota(jnp.int32, (rows, LANES), 0)

    def step(index, carry):
        at = pl.multiple_of(index * rows, rows)
        wave = waves_ref[pl.ds(at, rows), :].astype(F32)
        row = (local + at).astype(F32)
        within = row - chunk_rows * jnp.floor((row + 0.5) * (1.0 / chunk_rows))
        quarter = jnp.where(within > slots - 0.5, 0.25 * lon_count, 0.0)
        cosine, sine = turn(wave * lane + quarter, lon_count)
        step_cos, step_sin = turn(wave * float(LANES), lon_count)
        before = (cosine * step_cos + sine * step_sin) * norm_factor
        now = cosine * norm_factor
        twice = step_cos + step_cos
        for tile in range(lon_count // LANES):
            out_ref[pl.ds(at, rows), tile * LANES : (tile + 1) * LANES] = now.astype(BF16)
            before, now = now, twice * now - before
        return carry

    lax.fori_loop(0, waves_ref.shape[0] // rows, step, 0)


def weight_kernel(*refs):
    *near_refs, out_ref, held_ref = refs
    height = near_refs[0].shape[0]
    for turn_at, near_ref in enumerate(near_refs):
        held_ref[turn_at, :height, :] = near_ref[...]
    share = lax.rem(band_index(), SHARES)
    for place in range(SHARES):
        out_ref[place * height : (place + 1) * height, :] = held_ref[jnp.bitwise_xor(share, place), :height, :]


def turn(phase, period):
    phase = phase - period * jnp.floor(phase * (1.0 / period) + 0.5)
    quadrant = jnp.floor(phase * (4.0 / period) + 0.5)
    angle = (phase - quadrant * (0.25 * period)) * (2.0 * math.pi / period)
    sq = angle * angle
    cosine = 1.0 + sq * (-1.0 / 2 + sq * (1.0 / 24 + sq * (-1.0 / 720 + sq * (1.0 / 40320))))
    sine = angle * (1.0 + sq * (-1.0 / 6 + sq * (1.0 / 120 + sq * (-1.0 / 5040 + sq * (1.0 / 362880)))))
    odd = jnp.abs(quadrant) == 1.0
    cos_base = jnp.where(odd, -quadrant * sine, cosine)
    sin_base = jnp.where(odd, quadrant * cosine, sine)
    back = jnp.abs(quadrant) == 2.0
    return jnp.where(back, -cos_base, cos_base), jnp.where(back, -sin_base, sin_base)


def pieces_of(value):
    high = value.astype(BF16).astype(F32)
    middle = (value - high).astype(BF16).astype(F32)
    low = (value - high - middle).astype(BF16).astype(F32)
    return high, middle, low


def grid_kernel(x_ref, table_ref, weight_ref, norm_ref, out_ref, turned_ref, wide_ref):
    count, lons = table_ref.shape
    step = 256
    turned_ref[...] = x_ref[...].astype(F32).T.astype(BF16)
    energy = jnp.zeros((SUB, step), F32)
    for first in range(0, lons, step):
        cols = slice(first, first + step)
        grid = jnp.dot(turned_ref[...], table_ref[:, cols], preferred_element_type=F32)
        weight = weight_ref[:, cols]
        weighted = []
        for group in range(GROUPS):
            rows = grid[group * PIECE : (group + 1) * PIECE]
            product = weight * rows
            weighted.append(product)
            square = product * rows
            for block in range(0, PIECE, SUB):
                energy = energy + square[block : block + SUB]
        weighted.append(jnp.zeros((LANES - SPARE, step), F32))
        wide_ref[cols, :] = jnp.concatenate(weighted, axis=0).T.astype(BF16)
    lane = lane_of(1)
    spare = jnp.zeros((1, LANES), F32)
    values = pieces_of(jnp.sum(norm_ref[...], axis=(0, 1), keepdims=True))
    values = values + pieces_of(jnp.sum(energy, axis=(0, 1), keepdims=True))
    for place, value in enumerate(values):
        spare = jnp.where(lane == SPARE + place, value, spare)
    for first in range(0, count, step):
        rows = slice(first, first + step)
        back = jnp.dot(table_ref[rows, :], wide_ref[...], preferred_element_type=F32)
        out_ref[rows, :] = jnp.where(lane >= SPARE, spare, back).astype(BF16)


def tail_kernel(x_ref, out_ref):
    total = jnp.zeros((SUB, LANES), F32)
    block = 2 * SUB
    for first in range(0, x_ref.shape[0], block):
        value = x_ref[first : first + block, :].astype(F32)
        total = total + value[:SUB] + value[SUB:]
    out_ref[...] = total


def exchange(payload, parts):
    rows = payload.shape[0]
    packed = payload.reshape(parts, rows // parts // 2, 2, LANES)
    return lax.all_to_all(packed, BAND, 0, 0, tiled=True).reshape(rows, LANES)


def call(kernel, name, outs, ins, scratch=(), vmem=24, flops=2_000_000_000):
    return pl.pallas_call(
        kernel,
        in_specs=ins,
        out_specs=[pl.BlockSpec(memory_space=pltpu.VMEM)] * len(outs),
        out_shape=outs,
        scratch_shapes=scratch,
        compiler_params=pltpu.CompilerParams(vmem_limit_bytes=vmem * 1024 * 1024),
        cost_estimate=pl.CostEstimate(flops=flops, bytes_accessed=1_000_000, transcendentals=0),
        name=name,
    )


def on_device(right_side, legendre, wave_map, obs_weight):
    slots, degrees, lats = legendre.shape
    lon_count = obs_weight.shape[1]
    bands = ZS * YS * CS
    rows = bands * 2 * slots
    chunk_rows = 2 * slots
    smem = pl.BlockSpec(memory_space=pltpu.SMEM)
    vmem = pl.BlockSpec(memory_space=pltpu.VMEM)
    flat = right_side.reshape(-1, LANES)
    spread = jnp.broadcast_to(wave_map.reshape(bands, 1, slots), (bands, 2, slots)).reshape(rows, 1)
    spread = jnp.broadcast_to(spread, (rows, LANES))
    flat, spread = lax.optimization_barrier((flat, spread))

    vec_shape = jax.ShapeDtypeStruct((slots, GROUPS * SUB, degrees), F32)
    payload_shape = jax.ShapeDtypeStruct((rows, LANES), BF16)
    small_shape = jax.ShapeDtypeStruct((SUB, LANES), F32)
    flat_shape = jax.ShapeDtypeStruct(flat.shape, F32)
    held = pltpu.VMEM((rows, LANES), F32)

    (table,) = call(
        functools.partial(fourier_kernel, chunk_rows, slots, 1.0 / math.sqrt(wave_map.shape[0])),
        "fourier",
        [jax.ShapeDtypeStruct((rows, lon_count), BF16)],
        [vmem],
        flops=4_000_000_000,
    )(spread)
    flat, table = lax.optimization_barrier((flat, table))

    res, payload, norm = call(
        functools.partial(first_kernel, slots, chunk_rows),
        "first",
        [vec_shape, payload_shape, small_shape],
        [smem, vmem, vmem],
        [held, pltpu.VMEM((GROUPS * SUB, LANES), F32)],
    )(wave_map, flat, legendre)

    near = [obs_weight]
    for turn_at in range(1, SHARES):
        pairs = [(at, at ^ turn_at) for at in range(YS * CS)]
        near.append(lax.ppermute(obs_weight, ("y", "c"), pairs))
    (weight,) = call(
        weight_kernel,
        "weight",
        [jax.ShapeDtypeStruct((PIECE, lon_count), F32)],
        [vmem] * SHARES,
        [pltpu.VMEM((SHARES, 2 * SUB, lon_count), F32)],
    )(*near)
    payload, table, weight = lax.optimization_barrier((payload, table, weight))

    def reach(payload, norm):
        arrived = exchange(payload, bands)
        (back,) = call(
            grid_kernel,
            "grid",
            [payload_shape],
            [vmem] * 4,
            [pltpu.VMEM((LANES, rows), BF16), pltpu.VMEM((lon_count, LANES), BF16)],
        )(arrived, table, weight, norm)
        home = exchange(back, bands)
        (sums,) = call(tail_kernel, "tail", [small_shape], [vmem])(home)
        others = [lax.ppermute(sums, "x", [(i, (i + k) % XS) for i in range(XS)]) for k in range(1, XS)]
        (adjoint,) = call(
            functools.partial(back_kernel, slots, chunk_rows),
            "back",
            [vec_shape],
            [smem, vmem, vmem],
            [held],
            flops=8_000_000_000,
        )(wave_map, home, legendre)
        return adjoint, [sums] + others

    residuals = [res]
    carried = []
    for stage in range(2):
        adjoint, sums = reach(payload, norm)
        operands = [*sums, legendre, adjoint, residuals[-1], *carried]
        res, along, payload, norm, past = call(
            functools.partial(middle_kernel, stage, slots, chunk_rows),
            f"middle{stage}",
            [vec_shape, vec_shape, payload_shape, small_shape, small_shape],
            [vmem] * len(operands),
            [held],
        )(*operands)
        residuals.append(res)
        carried = [along, past]
    adjoint, sums = reach(payload, norm)
    solution, residual = call(
        functools.partial(last_kernel, slots, chunk_rows),
        "last",
        [flat_shape, flat_shape],
        [vmem] * 10,
        [pltpu.VMEM((2 * GROUPS * SUB * (degrees // LANES), LANES), F32)],
    )(*sums, adjoint, *residuals, along, past)
    return solution.reshape(right_side.shape), residual.reshape(right_side.shape)


def solution(mesh):
    split = Mesh(mesh.devices.reshape(ZS, YS, CS, XS), ("z", "y", "c", "x"))
    return jax.shard_map(
        on_device,
        mesh=split,
        in_specs=(P(BAND, None, "x", None, None), P(BAND, None, None), P(), P(BAND, None)),
        out_specs=(P(BAND, None, "x", None, None), P(BAND, None, "x", None, None)),
        check_vma=False,
    )
```

```python
import functools
import math

import jax
import jax.numpy as jnp
from jax import lax
from jax.experimental import pallas as pl
from jax.experimental.pallas import tpu as pltpu
from jax.sharding import Mesh
from jax.sharding import PartitionSpec as P

ZS, YS, CS, XS = 8, 4, 2, 4
BAND = ("z", "y", "c")
GROUPS = 3
SHARES = 4
PIECE = 40
PIECES = 16
SUB = 8
LANES = 128
SPARE = GROUPS * PIECE
F32 = jnp.float32
BF16 = jnp.bfloat16
UNROLL = 10


def lane_of(rows=SUB):
    return lax.broadcasted_iota(jnp.int32, (rows, LANES), 1)


def scatter_rows(value, acc_ref, slot, chunk_rows, slots):
    lane = lane_of()
    for piece in range(PIECES):
        first = piece * PIECE
        tile, offset = first // LANES, first % LANES
        out = jnp.zeros((SUB, LANES), F32)
        for group in reversed(range(GROUPS)):
            rows = slice(group * SUB, (group + 1) * SUB)
            source = value[rows, tile * LANES : (tile + 1) * LANES]
            if offset + PIECE > LANES:
                following = value[rows, (tile + 1) * LANES : (tile + 2) * LANES]
                source = jnp.where(lane >= offset, source, following)
            shift = (group * PIECE - offset) % LANES
            if shift:
                source = pltpu.roll(source, shift, 1)
            out = jnp.where(lane < (group + 1) * PIECE, source, out)
        acc_ref[pl.ds(piece * SHARES * chunk_rows + slot, SUB, stride=slots), :] = out


def gather_rows(held_ref, slot, chunk_rows, slots, lat_tiles):
    lane = lane_of()
    tiles = [[None] * lat_tiles for _ in range(GROUPS)]
    for piece in range(PIECES):
        first = piece * PIECE
        tile, offset = first // LANES, first % LANES
        rows = held_ref[pl.ds(piece * SHARES * chunk_rows + slot, SUB, stride=slots), :]
        for group in range(GROUPS):
            shift = (offset - group * PIECE) % LANES
            moved = pltpu.roll(rows, shift, 1) if shift else rows
            known = tiles[group][tile]
            tiles[group][tile] = moved if known is None else jnp.where(lane >= offset, moved, known)
            if offset + PIECE > LANES:
                tiles[group][tile + 1] = moved
    return jnp.concatenate([jnp.concatenate(row, axis=1) for row in tiles], axis=0)


def square_sum(parts):
    total = None
    for part in parts:
        for group in range(GROUPS):
            block = part[group * SUB : (group + 1) * SUB, :]
            total = block * block if total is None else total + block * block
    return total


def triangle_tile(wave, tile):
    return lane_of(GROUPS * SUB) + tile * LANES >= wave


def band_index():
    return (lax.axis_index("z") * YS + lax.axis_index("y")) * CS + lax.axis_index("c")


def wave_of(waves_ref, slots, slot):
    return waves_ref[band_index() * slots + slot]


def flat_rows(slot, group, tile, part, tiles):
    first = ((slot * 2 + part) * GROUPS + group) * SHARES * tiles + tile
    return pl.ds(first, SHARES, stride=tiles)


def first_kernel(slots, chunk_rows, waves_ref, vec_ref, leg_ref, res_ref, out_ref, norm_ref, acc_ref, turn_ref):
    tiles = leg_ref.shape[1] // LANES
    norm_ref[...] = jnp.zeros_like(norm_ref)

    def step(slot, carry):
        wave = wave_of(waves_ref, slots, slot)
        parts = []
        for tile in range(tiles):
            cols = slice(tile * LANES, (tile + 1) * LANES)
            for group in range(GROUPS):
                for part in range(2):
                    rows = vec_ref[flat_rows(slot, group, tile, part, tiles), :]
                    turn_ref[pl.ds(group * SUB + part, SHARES, stride=2), :] = rows
            parts.append(jnp.where(triangle_tile(wave, tile), turn_ref[...], 0.0))
            res_ref[slot, :, cols] = parts[-1]
        norm_ref[...] += square_sum(parts)
        forward(jnp.concatenate(parts, axis=1), leg_ref, acc_ref, slot, slots, chunk_rows)
        return carry

    lax.fori_loop(0, slots, step, 0, unroll=UNROLL)
    out_ref[...] = acc_ref[...].astype(BF16)


def forward(vector, leg_ref, acc_ref, slot, slots, chunk_rows):
    coeffs = jnp.dot(vector.astype(BF16), leg_ref[slot], preferred_element_type=F32)
    scatter_rows(coeffs, acc_ref, slot, chunk_rows, slots)


def sums_of(sum_refs, chunk_rows):
    total = sum_refs[0][...]
    for ref in sum_refs[1:]:
        total = total + ref[...]
    total = total * (1.0 / chunk_rows)
    lane = lane_of()
    norm = jnp.sum(jnp.where((lane >= SPARE) & (lane < SPARE + 3), total, 0.0), axis=(0, 1), keepdims=True)
    energy = jnp.sum(jnp.where((lane >= SPARE + 3) & (lane < SPARE + 6), total, 0.0), axis=(0, 1), keepdims=True)
    return norm, norm + energy


def back_kernel(slots, chunk_rows, waves_ref, home_ref, leg_ref, adj_ref, held_ref):
    held_ref[...] = home_ref[...].astype(F32)
    tiles = leg_ref.shape[2] // LANES

    def step(slot, carry):
        wave = wave_of(waves_ref, slots, slot)
        home = gather_rows(held_ref, slot, chunk_rows, slots, tiles).astype(BF16)
        adjoint = lax.dot_general(home, leg_ref[slot], (((1,), (1,)), ((), ())), preferred_element_type=F32)
        for tile in range(leg_ref.shape[1] // LANES):
            cols = slice(tile * LANES, (tile + 1) * LANES)
            adj_ref[slot, :, cols] = jnp.where(triangle_tile(wave, tile), adjoint[:, cols], 0.0)
        return carry

    lax.fori_loop(0, slots, step, 0, unroll=UNROLL)


def scalar_row(value):
    return jnp.broadcast_to(value, (1, LANES))


def middle_kernel(stage, slots, chunk_rows, *refs):
    if stage == 0:
        sum_a, sum_b, sum_c, sum_d, leg_ref, adj_ref, res_ref, *refs = refs
    else:
        sum_a, sum_b, sum_c, sum_d, leg_ref, adj_ref, res_ref, last_ref, past_ref, *refs = refs
    new_ref, along_ref, out_ref, norm_ref, hist_ref, acc_ref = refs
    norm, product = sums_of((sum_a, sum_b, sum_c, sum_d), chunk_rows)
    hist_ref[...] = jnp.zeros_like(hist_ref)
    if stage == 0:
        alpha = norm / product
        beta = jnp.zeros_like(norm)
        hist_ref[2:3, :] = scalar_row(alpha)
    else:
        beta = norm / past_ref[0:1, 0:1]
        alpha = norm / (product - beta * norm / past_ref[1:2, 0:1])
        hist_ref[2:3, :] = past_ref[2:3, :]
        hist_ref[3:4, :] = scalar_row(alpha)
    hist_ref[0:1, :] = scalar_row(norm)
    hist_ref[1:2, :] = scalar_row(alpha)
    hist_ref[4:5, :] = scalar_row(beta)
    norm_ref[...] = jnp.zeros_like(norm_ref)

    def step(slot, carry):
        alpha = hist_ref[1:2, :]
        beta = hist_ref[4:5, :]
        parts = []
        for tile in range(leg_ref.shape[1] // LANES):
            cols = slice(tile * LANES, (tile + 1) * LANES)
            res = res_ref[slot, :, cols]
            along = res + adj_ref[slot, :, cols]
            if stage > 0:
                along = along + beta * last_ref[slot, :, cols]
            along_ref[slot, :, cols] = along
            part = res - alpha * along
            new_ref[slot, :, cols] = part
            parts.append(part)
        norm_ref[...] += square_sum(parts)
        forward(jnp.concatenate(parts, axis=1), leg_ref, acc_ref, slot, slots, chunk_rows)
        return carry

    lax.fori_loop(0, slots, step, 0, unroll=UNROLL)
    out_ref[...] = acc_ref[...].astype(BF16)


def last_kernel(slots, chunk_rows, *refs):
    sum_a, sum_b, sum_c, sum_d, adj_ref, res0_ref, res1_ref, res2_ref, last_ref, past_ref, *refs = refs
    sol_hbm, fin_hbm, turn_ref, sol_ref, fin_ref, sol_sems, fin_sems = refs
    norm, product = sums_of((sum_a, sum_b, sum_c, sum_d), chunk_rows)
    beta = norm / past_ref[0:1, 0:1]
    alpha = scalar_row(norm / (product - beta * norm / past_ref[1:2, 0:1]))
    beta = scalar_row(beta)
    alpha0, alpha1, beta1 = past_ref[2:3, :], past_ref[3:4, :], past_ref[4:5, :]
    tiles = adj_ref.shape[2] // LANES
    height = GROUPS * SUB

    rows_each = sol_hbm.shape[0] // slots
    copies = []

    def send(slot):
        rows = pl.ds(slot * rows_each, rows_each)
        copies.append(pltpu.make_async_copy(sol_ref.at[rows], sol_hbm.at[rows], sol_sems.at[slot]))
        copies.append(pltpu.make_async_copy(fin_ref.at[rows], fin_hbm.at[rows], fin_sems.at[slot]))
        copies[-2].start()
        copies[-1].start()

    for slot in range(slots):
        for tile in range(tiles):
            cols = slice(tile * LANES, (tile + 1) * LANES)
            res2 = res2_ref[slot, :, cols]
            along = res2 + adj_ref[slot, :, cols] + beta * last_ref[slot, :, cols]
            first = res0_ref[slot, :, cols]
            second = res1_ref[slot, :, cols] + beta1 * first
            third = res2 + beta * second
            turn_ref[(2 * tile) * height : (2 * tile + 1) * height, :] = res2 - alpha * along
            turn_ref[(2 * tile + 1) * height : (2 * tile + 2) * height, :] = (
                alpha0 * first + alpha1 * second + alpha * third
            )
            for group in range(GROUPS):
                for part in range(2):
                    rows = flat_rows(slot, group, tile, part, tiles)
                    at = group * SUB + part
                    fin_ref[rows, :] = turn_ref[pl.ds((2 * tile) * height + at, SHARES, stride=2), :]
                    sol_ref[rows, :] = turn_ref[pl.ds((2 * tile + 1) * height + at, SHARES, stride=2), :]
        if slot > 0:
            send(slot - 1)
    send(slots - 1)
    for copy in copies:
        copy.wait()


def fourier_kernel(chunk_rows, slots, norm_factor, waves_ref, out_ref):
    rows = 32
    lon_count = out_ref.shape[1]
    lane = lax.broadcasted_iota(jnp.int32, (rows, LANES), 1).astype(F32)
    local = lax.broadcasted_iota(jnp.int32, (rows, LANES), 0)

    def step(index, carry):
        at = pl.multiple_of(index * rows, rows)
        wave = waves_ref[pl.ds(at, rows), :].astype(F32)
        row = (local + at).astype(F32)
        within = row - chunk_rows * jnp.floor((row + 0.5) * (1.0 / chunk_rows))
        quarter = jnp.where(within > slots - 0.5, 0.25 * lon_count, 0.0)
        cosine, sine = turn(wave * lane + quarter, lon_count)
        step_cos, step_sin = turn(wave * float(LANES), lon_count)
        before = (cosine * step_cos + sine * step_sin) * norm_factor
        now = cosine * norm_factor
        twice = step_cos + step_cos
        for tile in range(lon_count // LANES):
            out_ref[pl.ds(at, rows), tile * LANES : (tile + 1) * LANES] = now.astype(BF16)
            before, now = now, twice * now - before
        return carry

    lax.fori_loop(0, waves_ref.shape[0] // rows, step, 0)


def weight_kernel(*refs):
    *near_refs, out_ref, held_ref = refs
    height = near_refs[0].shape[0]
    for turn_at, near_ref in enumerate(near_refs):
        held_ref[turn_at, :height, :] = near_ref[...]
    share = lax.rem(band_index(), SHARES)
    for place in range(SHARES):
        out_ref[place * height : (place + 1) * height, :] = held_ref[jnp.bitwise_xor(share, place), :height, :]


def turn(phase, period):
    phase = phase - period * jnp.floor(phase * (1.0 / period) + 0.5)
    quadrant = jnp.floor(phase * (4.0 / period) + 0.5)
    angle = (phase - quadrant * (0.25 * period)) * (2.0 * math.pi / period)
    sq = angle * angle
    cosine = 1.0 + sq * (-1.0 / 2 + sq * (1.0 / 24 + sq * (-1.0 / 720 + sq * (1.0 / 40320))))
    sine = angle * (1.0 + sq * (-1.0 / 6 + sq * (1.0 / 120 + sq * (-1.0 / 5040 + sq * (1.0 / 362880)))))
    odd = jnp.abs(quadrant) == 1.0
    cos_base = jnp.where(odd, -quadrant * sine, cosine)
    sin_base = jnp.where(odd, quadrant * cosine, sine)
    back = jnp.abs(quadrant) == 2.0
    return jnp.where(back, -cos_base, cos_base), jnp.where(back, -sin_base, sin_base)


def pieces_of(value):
    high = value.astype(BF16).astype(F32)
    middle = (value - high).astype(BF16).astype(F32)
    low = (value - high - middle).astype(BF16).astype(F32)
    return high, middle, low


def grid_kernel(x_ref, table_ref, weight_ref, norm_ref, out_ref, turned_ref, wide_ref):
    count, lons = table_ref.shape
    step = 256
    turned_ref[...] = x_ref[...].T
    energy = jnp.zeros((SUB, step), F32)
    for first in range(0, lons, step):
        cols = slice(first, first + step)
        grid = jnp.dot(turned_ref[...], table_ref[:, cols], preferred_element_type=F32)
        weight = weight_ref[:, cols]
        weighted = []
        for group in range(GROUPS):
            rows = grid[group * PIECE : (group + 1) * PIECE]
            product = weight * rows
            weighted.append(product)
            square = product * rows
            for block in range(0, PIECE, SUB):
                energy = energy + square[block : block + SUB]
        weighted.append(jnp.zeros((LANES - SPARE, step), F32))
        wide_ref[:, cols] = jnp.concatenate(weighted, axis=0).astype(BF16)
    lane = lane_of(1)
    spare = jnp.zeros((1, LANES), F32)
    values = pieces_of(jnp.sum(norm_ref[...], axis=(0, 1), keepdims=True))
    values = values + pieces_of(jnp.sum(energy, axis=(0, 1), keepdims=True))
    for place, value in enumerate(values):
        spare = jnp.where(lane == SPARE + place, value, spare)
    for first in range(0, count, step):
        rows = slice(first, first + step)
        back = lax.dot_general(
            table_ref[rows, :], wide_ref[...], (((1,), (1,)), ((), ())), preferred_element_type=F32
        )
        out_ref[rows, :] = jnp.where(lane >= SPARE, spare, back).astype(BF16)


def tail_kernel(x_ref, out_ref):
    total = jnp.zeros((SUB, LANES), F32)
    block = 2 * SUB
    for first in range(0, x_ref.shape[0], block):
        value = x_ref[first : first + block, :].astype(F32)
        total = total + value[:SUB] + value[SUB:]
    out_ref[...] = total


def exchange(payload, parts):
    rows = payload.shape[0]
    packed = payload.reshape(parts, rows // parts // 2, 2, LANES)
    return lax.all_to_all(packed, BAND, 0, 0, tiled=True).reshape(rows, LANES)


def call(kernel, name, outs, ins, scratch=(), vmem=24, flops=2_000_000_000, place=pltpu.VMEM):
    return pl.pallas_call(
        kernel,
        in_specs=ins,
        out_specs=[pl.BlockSpec(memory_space=place)] * len(outs),
        out_shape=outs,
        scratch_shapes=scratch,
        compiler_params=pltpu.CompilerParams(vmem_limit_bytes=vmem * 1024 * 1024),
        cost_estimate=pl.CostEstimate(flops=flops, bytes_accessed=1_000_000, transcendentals=0),
        name=name,
    )


def on_device(right_side, legendre, wave_map, obs_weight):
    slots, degrees, lats = legendre.shape
    lon_count = obs_weight.shape[1]
    bands = ZS * YS * CS
    rows = bands * 2 * slots
    chunk_rows = 2 * slots
    smem = pl.BlockSpec(memory_space=pltpu.SMEM)
    vmem = pl.BlockSpec(memory_space=pltpu.VMEM)
    flat = right_side.reshape(-1, LANES)
    spread = jnp.broadcast_to(wave_map.reshape(bands, 1, slots), (bands, 2, slots)).reshape(rows, 1)
    spread = jnp.broadcast_to(spread, (rows, LANES))
    flat, spread = lax.optimization_barrier((flat, spread))

    vec_shape = jax.ShapeDtypeStruct((slots, GROUPS * SUB, degrees), F32)
    payload_shape = jax.ShapeDtypeStruct((rows, LANES), BF16)
    small_shape = jax.ShapeDtypeStruct((SUB, LANES), F32)
    flat_shape = jax.ShapeDtypeStruct(flat.shape, F32)
    held = pltpu.VMEM((rows, LANES), F32)

    (table,) = call(
        functools.partial(fourier_kernel, chunk_rows, slots, 1.0 / math.sqrt(wave_map.shape[0])),
        "fourier",
        [jax.ShapeDtypeStruct((rows, lon_count), BF16)],
        [vmem],
        flops=4_000_000_000,
    )(spread)
    flat, table = lax.optimization_barrier((flat, table))

    res, payload, norm = call(
        functools.partial(first_kernel, slots, chunk_rows),
        "first",
        [vec_shape, payload_shape, small_shape],
        [smem, vmem, vmem],
        [held, pltpu.VMEM((GROUPS * SUB, LANES), F32)],
    )(wave_map, flat, legendre)

    near = [obs_weight]
    for turn_at in range(1, SHARES):
        pairs = [(at, at ^ turn_at) for at in range(YS * CS)]
        near.append(lax.ppermute(obs_weight, ("y", "c"), pairs))
    (weight,) = call(
        weight_kernel,
        "weight",
        [jax.ShapeDtypeStruct((PIECE, lon_count), F32)],
        [vmem] * SHARES,
        [pltpu.VMEM((SHARES, 2 * SUB, lon_count), F32)],
    )(*near)
    payload, table, weight = lax.optimization_barrier((payload, table, weight))

    def reach(payload, norm):
        arrived = exchange(payload, bands)
        (back,) = call(
            grid_kernel,
            "grid",
            [payload_shape],
            [vmem] * 4,
            [pltpu.VMEM((LANES, rows), BF16), pltpu.VMEM((LANES, lon_count), BF16)],
        )(arrived, table, weight, norm)
        home = exchange(back, bands)
        (sums,) = call(tail_kernel, "tail", [small_shape], [vmem])(home)
        others = [lax.ppermute(sums, "x", [(i, (i + k) % XS) for i in range(XS)]) for k in range(1, XS)]
        (adjoint,) = call(
            functools.partial(back_kernel, slots, chunk_rows),
            "back",
            [vec_shape],
            [smem, vmem, vmem],
            [held],
            flops=8_000_000_000,
        )(wave_map, home, legendre)
        return adjoint, [sums] + others

    residuals = [res]
    carried = []
    for stage in range(2):
        adjoint, sums = reach(payload, norm)
        operands = [*sums, legendre, adjoint, residuals[-1], *carried]
        res, along, payload, norm, past = call(
            functools.partial(middle_kernel, stage, slots, chunk_rows),
            f"middle{stage}",
            [vec_shape, vec_shape, payload_shape, small_shape, small_shape],
            [vmem] * len(operands),
            [held],
        )(*operands)
        residuals.append(res)
        carried = [along, past]
    adjoint, sums = reach(payload, norm)
    solution, residual = call(
        functools.partial(last_kernel, slots, chunk_rows),
        "last",
        [flat_shape, flat_shape],
        [vmem] * 10,
        [
            pltpu.VMEM((2 * GROUPS * SUB * (degrees // LANES), LANES), F32),
            pltpu.VMEM(flat.shape, F32),
            pltpu.VMEM(flat.shape, F32),
            pltpu.SemaphoreType.DMA((slots,)),
            pltpu.SemaphoreType.DMA((slots,)),
        ],
        place=pltpu.HBM,
    )(*sums, adjoint, *residuals, along, past)
    return solution.reshape(right_side.shape), residual.reshape(right_side.shape)


def solution(mesh):
    split = Mesh(mesh.devices.reshape(ZS, YS, CS, XS), ("z", "y", "c", "x"))
    return jax.shard_map(
        on_device,
        mesh=split,
        in_specs=(P(BAND, None, "x", None, None), P(BAND, None, None), P(), P(BAND, None)),
        out_specs=(P(BAND, None, "x", None, None), P(BAND, None, "x", None, None)),
        check_vma=False,
    )
```

```python
import functools
import math

import jax
import jax.numpy as jnp
from jax import lax
from jax.experimental import pallas as pl
from jax.experimental.pallas import tpu as pltpu
from jax.sharding import Mesh
from jax.sharding import PartitionSpec as P

ZS, YS, CS, XS = 8, 4, 2, 4
BAND = ("z", "y", "c")
GROUPS = 3
SHARES = 4
PIECE = 40
PIECES = 16
SUB = 8
LANES = 128
SPARE = GROUPS * PIECE
F32 = jnp.float32
BF16 = jnp.bfloat16
UNROLL = 10


def lane_of(rows=SUB):
    return lax.broadcasted_iota(jnp.int32, (rows, LANES), 1)


def scatter_rows(value, acc_ref, slot, chunk_rows, slots):
    lane = lane_of()
    for piece in range(PIECES):
        first = piece * PIECE
        tile, offset = first // LANES, first % LANES
        out = jnp.zeros((SUB, LANES), F32)
        for group in reversed(range(GROUPS)):
            rows = slice(group * SUB, (group + 1) * SUB)
            source = value[rows, tile * LANES : (tile + 1) * LANES]
            if offset + PIECE > LANES:
                following = value[rows, (tile + 1) * LANES : (tile + 2) * LANES]
                source = jnp.where(lane >= offset, source, following)
            shift = (group * PIECE - offset) % LANES
            if shift:
                source = pltpu.roll(source, shift, 1)
            out = jnp.where(lane < (group + 1) * PIECE, source, out)
        acc_ref[pl.ds(piece * SHARES * chunk_rows + slot, SUB, stride=slots), :] = out


def gather_rows(held_ref, slot, chunk_rows, slots, lat_tiles):
    lane = lane_of()
    tiles = [[None] * lat_tiles for _ in range(GROUPS)]
    for piece in range(PIECES):
        first = piece * PIECE
        tile, offset = first // LANES, first % LANES
        rows = held_ref[pl.ds(piece * SHARES * chunk_rows + slot, SUB, stride=slots), :]
        for group in range(GROUPS):
            shift = (offset - group * PIECE) % LANES
            moved = pltpu.roll(rows, shift, 1) if shift else rows
            known = tiles[group][tile]
            tiles[group][tile] = moved if known is None else jnp.where(lane >= offset, moved, known)
            if offset + PIECE > LANES:
                tiles[group][tile + 1] = moved
    return jnp.concatenate([jnp.concatenate(row, axis=1) for row in tiles], axis=0)


def square_sum(parts):
    total = None
    for part in parts:
        for group in range(GROUPS):
            block = part[group * SUB : (group + 1) * SUB, :]
            total = block * block if total is None else total + block * block
    return total


def triangle_tile(wave, tile):
    return lane_of(GROUPS * SUB) + tile * LANES >= wave


def band_index():
    return (lax.axis_index("z") * YS + lax.axis_index("y")) * CS + lax.axis_index("c")


def wave_of(waves_ref, slots, slot):
    return waves_ref[band_index() * slots + slot]


def flat_rows(slot, group, tile, part, tiles):
    first = ((slot * 2 + part) * GROUPS + group) * SHARES * tiles + tile
    return pl.ds(first, SHARES, stride=tiles)


def first_kernel(slots, chunk_rows, waves_ref, vec_ref, leg_ref, res_ref, out_ref, norm_ref, acc_ref, turn_ref):
    tiles = leg_ref.shape[1] // LANES
    norm_ref[...] = jnp.zeros_like(norm_ref)

    def step(slot, carry):
        wave = wave_of(waves_ref, slots, slot)
        parts = []
        for tile in range(tiles):
            cols = slice(tile * LANES, (tile + 1) * LANES)
            for group in range(GROUPS):
                for part in range(2):
                    rows = vec_ref[flat_rows(slot, group, tile, part, tiles), :]
                    turn_ref[pl.ds(group * SUB + part, SHARES, stride=2), :] = rows
            parts.append(jnp.where(triangle_tile(wave, tile), turn_ref[...], 0.0))
            res_ref[slot, :, cols] = parts[-1]
        norm_ref[...] += square_sum(parts)
        forward(jnp.concatenate(parts, axis=1), leg_ref, acc_ref, slot, slots, chunk_rows)
        return carry

    lax.fori_loop(0, slots, step, 0, unroll=UNROLL)
    out_ref[...] = acc_ref[...].astype(BF16)


def forward(vector, leg_ref, acc_ref, slot, slots, chunk_rows):
    coeffs = jnp.dot(vector.astype(BF16), leg_ref[slot], preferred_element_type=F32)
    scatter_rows(coeffs, acc_ref, slot, chunk_rows, slots)


def sums_of(sum_refs, chunk_rows):
    total = sum_refs[0][...]
    for ref in sum_refs[1:]:
        total = total + ref[...]
    total = total * (1.0 / chunk_rows)
    lane = lane_of()
    norm = jnp.sum(jnp.where((lane >= SPARE) & (lane < SPARE + 3), total, 0.0), axis=(0, 1), keepdims=True)
    energy = jnp.sum(jnp.where((lane >= SPARE + 3) & (lane < SPARE + 6), total, 0.0), axis=(0, 1), keepdims=True)
    return norm, norm + energy


def back_kernel(slots, chunk_rows, waves_ref, home_ref, leg_ref, adj_ref, held_ref):
    held_ref[...] = home_ref[...].astype(F32)
    tiles = leg_ref.shape[2] // LANES

    def step(slot, carry):
        wave = wave_of(waves_ref, slots, slot)
        home = gather_rows(held_ref, slot, chunk_rows, slots, tiles).astype(BF16)
        adjoint = lax.dot_general(home, leg_ref[slot], (((1,), (1,)), ((), ())), preferred_element_type=F32)
        for tile in range(leg_ref.shape[1] // LANES):
            cols = slice(tile * LANES, (tile + 1) * LANES)
            adj_ref[slot, :, cols] = jnp.where(triangle_tile(wave, tile), adjoint[:, cols], 0.0)
        return carry

    lax.fori_loop(0, slots, step, 0, unroll=UNROLL)


def scalar_row(value):
    return jnp.broadcast_to(value, (1, LANES))


def middle_kernel(stage, slots, chunk_rows, *refs):
    if stage == 0:
        sum_a, sum_b, sum_c, sum_d, leg_ref, adj_ref, res_ref, *refs = refs
    else:
        sum_a, sum_b, sum_c, sum_d, leg_ref, adj_ref, res_ref, last_ref, past_ref, *refs = refs
    new_ref, along_ref, out_ref, norm_ref, hist_ref, acc_ref = refs
    norm, product = sums_of((sum_a, sum_b, sum_c, sum_d), chunk_rows)
    hist_ref[...] = jnp.zeros_like(hist_ref)
    if stage == 0:
        alpha = norm / product
        beta = jnp.zeros_like(norm)
        hist_ref[2:3, :] = scalar_row(alpha)
    else:
        beta = norm / past_ref[0:1, 0:1]
        alpha = norm / (product - beta * norm / past_ref[1:2, 0:1])
        hist_ref[2:3, :] = past_ref[2:3, :]
        hist_ref[3:4, :] = scalar_row(alpha)
    hist_ref[0:1, :] = scalar_row(norm)
    hist_ref[1:2, :] = scalar_row(alpha)
    hist_ref[4:5, :] = scalar_row(beta)
    norm_ref[...] = jnp.zeros_like(norm_ref)

    def step(slot, carry):
        alpha = hist_ref[1:2, :]
        beta = hist_ref[4:5, :]
        parts = []
        for tile in range(leg_ref.shape[1] // LANES):
            cols = slice(tile * LANES, (tile + 1) * LANES)
            res = res_ref[slot, :, cols]
            along = res + adj_ref[slot, :, cols]
            if stage > 0:
                along = along + beta * last_ref[slot, :, cols]
            along_ref[slot, :, cols] = along
            part = res - alpha * along
            new_ref[slot, :, cols] = part
            parts.append(part)
        norm_ref[...] += square_sum(parts)
        forward(jnp.concatenate(parts, axis=1), leg_ref, acc_ref, slot, slots, chunk_rows)
        return carry

    lax.fori_loop(0, slots, step, 0, unroll=UNROLL)
    out_ref[...] = acc_ref[...].astype(BF16)


def last_kernel(slots, chunk_rows, *refs):
    sum_a, sum_b, sum_c, sum_d, adj_ref, res0_ref, res1_ref, res2_ref, last_ref, past_ref, *refs = refs
    sol_hbm, fin_hbm, turn_ref, sol_ref, fin_ref, sol_sems, fin_sems = refs
    norm, product = sums_of((sum_a, sum_b, sum_c, sum_d), chunk_rows)
    beta = norm / past_ref[0:1, 0:1]
    alpha = scalar_row(norm / (product - beta * norm / past_ref[1:2, 0:1]))
    beta = scalar_row(beta)
    alpha0, alpha1, beta1 = past_ref[2:3, :], past_ref[3:4, :], past_ref[4:5, :]
    tiles = adj_ref.shape[2] // LANES
    height = GROUPS * SUB

    rows_each = sol_hbm.shape[0] // slots
    copies = []

    def send(slot):
        rows = pl.ds(slot * rows_each, rows_each)
        copies.append(pltpu.make_async_copy(sol_ref.at[rows], sol_hbm.at[rows], sol_sems.at[slot]))
        copies.append(pltpu.make_async_copy(fin_ref.at[rows], fin_hbm.at[rows], fin_sems.at[slot]))
        copies[-2].start()
        copies[-1].start()

    for slot in range(slots):
        for tile in range(tiles):
            cols = slice(tile * LANES, (tile + 1) * LANES)
            res2 = res2_ref[slot, :, cols]
            along = res2 + adj_ref[slot, :, cols] + beta * last_ref[slot, :, cols]
            first = res0_ref[slot, :, cols]
            second = res1_ref[slot, :, cols] + beta1 * first
            third = res2 + beta * second
            turn_ref[(2 * tile) * height : (2 * tile + 1) * height, :] = res2 - alpha * along
            turn_ref[(2 * tile + 1) * height : (2 * tile + 2) * height, :] = (
                alpha0 * first + alpha1 * second + alpha * third
            )
            for group in range(GROUPS):
                for part in range(2):
                    rows = flat_rows(slot, group, tile, part, tiles)
                    at = group * SUB + part
                    fin_ref[rows, :] = turn_ref[pl.ds((2 * tile) * height + at, SHARES, stride=2), :]
                    sol_ref[rows, :] = turn_ref[pl.ds((2 * tile + 1) * height + at, SHARES, stride=2), :]
        if slot > 0:
            send(slot - 1)
    send(slots - 1)
    for copy in copies:
        copy.wait()


def fourier_kernel(chunk_rows, slots, norm_factor, map_ref, out_ref, column_ref, waves_ref):
    rows = 32
    lon_count = out_ref.shape[1]
    blocks = map_ref.shape[0]
    compact = jnp.concatenate([map_ref[...].astype(F32), jnp.zeros((SUB - blocks, LANES), F32)], axis=0)
    columns = jnp.concatenate([compact, jnp.zeros((LANES - SUB, LANES), F32)], axis=0).T
    for block in range(blocks):
        column_ref[block * LANES : (block + 1) * LANES, :] = jnp.broadcast_to(
            columns[:, block : block + 1], (LANES, LANES)
        )
    for band in range(waves_ref.shape[0] // chunk_rows):
        wave = column_ref[band * slots : (band + 1) * slots, :]
        for part in range(2):
            at = band * chunk_rows + part * slots
            waves_ref[at : at + slots, :] = wave
    lane = lax.broadcasted_iota(jnp.int32, (rows, LANES), 1).astype(F32)
    local = lax.broadcasted_iota(jnp.int32, (rows, LANES), 0)

    def step(index, carry):
        at = pl.multiple_of(index * rows, rows)
        wave = waves_ref[pl.ds(at, rows), :]
        row = (local + at).astype(F32)
        within = row - chunk_rows * jnp.floor((row + 0.5) * (1.0 / chunk_rows))
        quarter = jnp.where(within > slots - 0.5, 0.25 * lon_count, 0.0)
        cosine, sine = turn(wave * lane + quarter, lon_count)
        step_cos, step_sin = turn(wave * float(LANES), lon_count)
        before = (cosine * step_cos + sine * step_sin) * norm_factor
        now = cosine * norm_factor
        twice = step_cos + step_cos
        for tile in range(lon_count // LANES):
            out_ref[pl.ds(at, rows), tile * LANES : (tile + 1) * LANES] = now.astype(BF16)
            before, now = now, twice * now - before
        return carry

    lax.fori_loop(0, waves_ref.shape[0] // rows, step, 0)


def weight_kernel(*refs):
    *near_refs, out_ref, held_ref = refs
    height = near_refs[0].shape[0]
    for turn_at, near_ref in enumerate(near_refs):
        held_ref[turn_at, :height, :] = near_ref[...]
    share = lax.rem(band_index(), SHARES)
    for place in range(SHARES):
        out_ref[place * height : (place + 1) * height, :] = held_ref[jnp.bitwise_xor(share, place), :height, :]


def turn(phase, period):
    phase = phase - period * jnp.floor(phase * (1.0 / period) + 0.5)
    quadrant = jnp.floor(phase * (4.0 / period) + 0.5)
    angle = (phase - quadrant * (0.25 * period)) * (2.0 * math.pi / period)
    sq = angle * angle
    cosine = 1.0 + sq * (-1.0 / 2 + sq * (1.0 / 24 + sq * (-1.0 / 720 + sq * (1.0 / 40320))))
    sine = angle * (1.0 + sq * (-1.0 / 6 + sq * (1.0 / 120 + sq * (-1.0 / 5040 + sq * (1.0 / 362880)))))
    odd = jnp.abs(quadrant) == 1.0
    cos_base = jnp.where(odd, -quadrant * sine, cosine)
    sin_base = jnp.where(odd, quadrant * cosine, sine)
    back = jnp.abs(quadrant) == 2.0
    return jnp.where(back, -cos_base, cos_base), jnp.where(back, -sin_base, sin_base)


def pieces_of(value):
    high = value.astype(BF16).astype(F32)
    middle = (value - high).astype(BF16).astype(F32)
    low = (value - high - middle).astype(BF16).astype(F32)
    return high, middle, low


def grid_kernel(x_ref, table_ref, weight_ref, norm_ref, out_ref, turned_ref, wide_ref):
    count, lons = table_ref.shape
    step = 256
    turned_ref[...] = x_ref[...].T
    energy = jnp.zeros((SUB, step), F32)
    for first in range(0, lons, step):
        cols = slice(first, first + step)
        grid = jnp.dot(turned_ref[...], table_ref[:, cols], preferred_element_type=F32)
        weight = weight_ref[:, cols]
        weighted = []
        for group in range(GROUPS):
            rows = grid[group * PIECE : (group + 1) * PIECE]
            product = weight * rows
            weighted.append(product)
            square = product * rows
            for block in range(0, PIECE, SUB):
                energy = energy + square[block : block + SUB]
        weighted.append(jnp.zeros((LANES - SPARE, step), F32))
        wide_ref[:, cols] = jnp.concatenate(weighted, axis=0).astype(BF16)
    lane = lane_of(1)
    spare = jnp.zeros((1, LANES), F32)
    values = pieces_of(jnp.sum(norm_ref[...], axis=(0, 1), keepdims=True))
    values = values + pieces_of(jnp.sum(energy, axis=(0, 1), keepdims=True))
    for place, value in enumerate(values):
        spare = jnp.where(lane == SPARE + place, value, spare)
    for first in range(0, count, step):
        rows = slice(first, first + step)
        back = lax.dot_general(
            table_ref[rows, :], wide_ref[...], (((1,), (1,)), ((), ())), preferred_element_type=F32
        )
        out_ref[rows, :] = jnp.where(lane >= SPARE, spare, back).astype(BF16)


def tail_kernel(x_ref, out_ref):
    total = jnp.zeros((SUB, LANES), F32)
    block = 2 * SUB
    for first in range(0, x_ref.shape[0], block):
        value = x_ref[first : first + block, :].astype(F32)
        total = total + value[:SUB] + value[SUB:]
    out_ref[...] = total


def exchange(payload, parts):
    rows = payload.shape[0]
    packed = payload.reshape(parts, rows // parts // 2, 2, LANES)
    return lax.all_to_all(packed, BAND, 0, 0, tiled=True).reshape(rows, LANES)


def call(kernel, name, outs, ins, scratch=(), vmem=24, flops=2_000_000_000, place=pltpu.VMEM):
    return pl.pallas_call(
        kernel,
        in_specs=ins,
        out_specs=[pl.BlockSpec(memory_space=place)] * len(outs),
        out_shape=outs,
        scratch_shapes=scratch,
        compiler_params=pltpu.CompilerParams(vmem_limit_bytes=vmem * 1024 * 1024),
        cost_estimate=pl.CostEstimate(flops=flops, bytes_accessed=1_000_000, transcendentals=0),
        name=name,
    )


def on_device(right_side, legendre, wave_map, obs_weight):
    slots, degrees, lats = legendre.shape
    lon_count = obs_weight.shape[1]
    bands = ZS * YS * CS
    rows = bands * 2 * slots
    chunk_rows = 2 * slots
    smem = pl.BlockSpec(memory_space=pltpu.SMEM)
    vmem = pl.BlockSpec(memory_space=pltpu.VMEM)
    flat = right_side.reshape(-1, LANES)
    vec_shape = jax.ShapeDtypeStruct((slots, GROUPS * SUB, degrees), F32)
    payload_shape = jax.ShapeDtypeStruct((rows, LANES), BF16)
    small_shape = jax.ShapeDtypeStruct((SUB, LANES), F32)
    flat_shape = jax.ShapeDtypeStruct(flat.shape, F32)
    held = pltpu.VMEM((rows, LANES), F32)

    (table,) = call(
        functools.partial(fourier_kernel, chunk_rows, slots, 1.0 / math.sqrt(wave_map.shape[0])),
        "fourier",
        [jax.ShapeDtypeStruct((rows, lon_count), BF16)],
        [vmem],
        [pltpu.VMEM((wave_map.shape[0], LANES), F32), pltpu.VMEM((rows, LANES), F32)],
        flops=4_000_000_000,
    )(wave_map.reshape(-1, LANES))
    flat, table = lax.optimization_barrier((flat, table))

    res, payload, norm = call(
        functools.partial(first_kernel, slots, chunk_rows),
        "first",
        [vec_shape, payload_shape, small_shape],
        [smem, vmem, vmem],
        [held, pltpu.VMEM((GROUPS * SUB, LANES), F32)],
    )(wave_map, flat, legendre)

    near = [obs_weight]
    for turn_at in range(1, SHARES):
        pairs = [(at, at ^ turn_at) for at in range(YS * CS)]
        near.append(lax.ppermute(obs_weight, ("y", "c"), pairs))
    (weight,) = call(
        weight_kernel,
        "weight",
        [jax.ShapeDtypeStruct((PIECE, lon_count), F32)],
        [vmem] * SHARES,
        [pltpu.VMEM((SHARES, 2 * SUB, lon_count), F32)],
    )(*near)
    payload, table, weight = lax.optimization_barrier((payload, table, weight))

    def reach(payload, norm):
        arrived = exchange(payload, bands)
        (back,) = call(
            grid_kernel,
            "grid",
            [payload_shape],
            [vmem] * 4,
            [pltpu.VMEM((LANES, rows), BF16), pltpu.VMEM((LANES, lon_count), BF16)],
        )(arrived, table, weight, norm)
        home = exchange(back, bands)
        (sums,) = call(tail_kernel, "tail", [small_shape], [vmem])(home)
        others = [lax.ppermute(sums, "x", [(i, i ^ k) for i in range(XS)]) for k in range(1, XS)]
        (adjoint,) = call(
            functools.partial(back_kernel, slots, chunk_rows),
            "back",
            [vec_shape],
            [smem, vmem, vmem],
            [held],
            flops=8_000_000_000,
        )(wave_map, home, legendre)
        return adjoint, [sums] + others

    residuals = [res]
    carried = []
    for stage in range(2):
        adjoint, sums = reach(payload, norm)
        operands = [*sums, legendre, adjoint, residuals[-1], *carried]
        res, along, payload, norm, past = call(
            functools.partial(middle_kernel, stage, slots, chunk_rows),
            f"middle{stage}",
            [vec_shape, vec_shape, payload_shape, small_shape, small_shape],
            [vmem] * len(operands),
            [held],
        )(*operands)
        residuals.append(res)
        carried = [along, past]
    adjoint, sums = reach(payload, norm)
    solution, residual = call(
        functools.partial(last_kernel, slots, chunk_rows),
        "last",
        [flat_shape, flat_shape],
        [vmem] * 10,
        [
            pltpu.VMEM((2 * GROUPS * SUB * (degrees // LANES), LANES), F32),
            pltpu.VMEM(flat.shape, F32),
            pltpu.VMEM(flat.shape, F32),
            pltpu.SemaphoreType.DMA((slots,)),
            pltpu.SemaphoreType.DMA((slots,)),
        ],
        place=pltpu.HBM,
    )(*sums, adjoint, *residuals, along, past)
    return solution.reshape(right_side.shape), residual.reshape(right_side.shape)


def solution(mesh):
    split = Mesh(mesh.devices.reshape(ZS, YS, CS, XS), ("z", "y", "c", "x"))
    return jax.shard_map(
        on_device,
        mesh=split,
        in_specs=(P(BAND, None, "x", None, None), P(BAND, None, None), P(), P(BAND, None)),
        out_specs=(P(BAND, None, "x", None, None), P(BAND, None, "x", None, None)),
        check_vma=False,
    )
```

```python
import functools
import math

import jax
import jax.numpy as jnp
from jax import lax
from jax.experimental import pallas as pl
from jax.experimental.pallas import tpu as pltpu
from jax.sharding import Mesh
from jax.sharding import PartitionSpec as P

ZS, YS, CS, XS = 8, 4, 2, 4
BAND = ("z", "y", "c")
GROUPS = 3
SHARES = 4
PIECE = 40
PIECES = 16
SUB = 8
LANES = 128
SPARE = GROUPS * PIECE
F32 = jnp.float32
BF16 = jnp.bfloat16
UNROLL = 10


def lane_of(rows=SUB):
    return lax.broadcasted_iota(jnp.int32, (rows, LANES), 1)


def scatter_rows(value, acc_ref, slot, chunk_rows, slots):
    lane = lane_of()
    for piece in range(PIECES):
        first = piece * PIECE
        tile, offset = first // LANES, first % LANES
        out = jnp.zeros((SUB, LANES), F32)
        for group in reversed(range(GROUPS)):
            rows = slice(group * SUB, (group + 1) * SUB)
            source = value[rows, tile * LANES : (tile + 1) * LANES]
            if offset + PIECE > LANES:
                following = value[rows, (tile + 1) * LANES : (tile + 2) * LANES]
                source = jnp.where(lane >= offset, source, following)
            shift = (group * PIECE - offset) % LANES
            if shift:
                source = pltpu.roll(source, shift, 1)
            out = jnp.where(lane < (group + 1) * PIECE, source, out)
        acc_ref[pl.ds(piece * SHARES * chunk_rows + slot, SUB, stride=slots), :] = out


def gather_rows(held_ref, slot, chunk_rows, slots, lat_tiles):
    lane = lane_of()
    tiles = [[None] * lat_tiles for _ in range(GROUPS)]
    for piece in range(PIECES):
        first = piece * PIECE
        tile, offset = first // LANES, first % LANES
        rows = held_ref[pl.ds(piece * SHARES * chunk_rows + slot, SUB, stride=slots), :]
        for group in range(GROUPS):
            shift = (offset - group * PIECE) % LANES
            moved = pltpu.roll(rows, shift, 1) if shift else rows
            known = tiles[group][tile]
            tiles[group][tile] = moved if known is None else jnp.where(lane >= offset, moved, known)
            if offset + PIECE > LANES:
                tiles[group][tile + 1] = moved
    return jnp.concatenate([jnp.concatenate(row, axis=1) for row in tiles], axis=0)


def square_sum(parts):
    total = None
    for part in parts:
        for group in range(GROUPS):
            block = part[group * SUB : (group + 1) * SUB, :]
            total = block * block if total is None else total + block * block
    return total


def triangle_tile(wave, tile):
    return lane_of(GROUPS * SUB) + tile * LANES >= wave


def band_index():
    return (lax.axis_index("z") * YS + lax.axis_index("y")) * CS + lax.axis_index("c")


def wave_of(waves_ref, slots, slot):
    return waves_ref[band_index() * slots + slot]


def flat_rows(slot, group, tile, part, tiles):
    first = ((slot * 2 + part) * GROUPS + group) * SHARES * tiles + tile
    return pl.ds(first, SHARES, stride=tiles)


def first_kernel(slots, chunk_rows, waves_ref, vec_ref, leg_ref, res_ref, out_ref, norm_ref, acc_ref, turn_ref):
    tiles = leg_ref.shape[1] // LANES
    norm_ref[...] = jnp.zeros_like(norm_ref)

    def step(slot, carry):
        wave = wave_of(waves_ref, slots, slot)
        parts = []
        for tile in range(tiles):
            cols = slice(tile * LANES, (tile + 1) * LANES)
            for group in range(GROUPS):
                for part in range(2):
                    rows = vec_ref[flat_rows(slot, group, tile, part, tiles), :]
                    turn_ref[pl.ds(group * SUB + part, SHARES, stride=2), :] = rows
            parts.append(jnp.where(triangle_tile(wave, tile), turn_ref[...], 0.0))
            res_ref[slot, :, cols] = parts[-1]
        norm_ref[...] += square_sum(parts)
        forward(jnp.concatenate(parts, axis=1), leg_ref, acc_ref, slot, slots, chunk_rows)
        return carry

    lax.fori_loop(0, slots, step, 0, unroll=UNROLL)
    out_ref[...] = acc_ref[...].astype(BF16)


def forward(vector, leg_ref, acc_ref, slot, slots, chunk_rows):
    coeffs = jnp.dot(vector.astype(BF16), leg_ref[slot], preferred_element_type=F32)
    scatter_rows(coeffs, acc_ref, slot, chunk_rows, slots)


def sums_of(sum_refs, chunk_rows):
    total = sum_refs[0][...]
    for ref in sum_refs[1:]:
        total = total + ref[...]
    total = total * (1.0 / chunk_rows)
    lane = lane_of()
    norm = jnp.sum(jnp.where((lane >= SPARE) & (lane < SPARE + 3), total, 0.0), axis=(0, 1), keepdims=True)
    energy = jnp.sum(jnp.where((lane >= SPARE + 3) & (lane < SPARE + 6), total, 0.0), axis=(0, 1), keepdims=True)
    return norm, norm + energy


def back_kernel(slots, chunk_rows, waves_ref, home_ref, leg_ref, adj_ref, held_ref):
    held_ref[...] = home_ref[...].astype(F32)
    tiles = leg_ref.shape[2] // LANES

    def step(slot, carry):
        wave = wave_of(waves_ref, slots, slot)
        home = gather_rows(held_ref, slot, chunk_rows, slots, tiles).astype(BF16)
        adjoint = lax.dot_general(home, leg_ref[slot], (((1,), (1,)), ((), ())), preferred_element_type=F32)
        for tile in range(leg_ref.shape[1] // LANES):
            cols = slice(tile * LANES, (tile + 1) * LANES)
            adj_ref[slot, :, cols] = jnp.where(triangle_tile(wave, tile), adjoint[:, cols], 0.0)
        return carry

    lax.fori_loop(0, slots, step, 0, unroll=UNROLL)


def scalar_row(value):
    return jnp.broadcast_to(value, (1, LANES))


def middle_kernel(stage, slots, chunk_rows, *refs):
    if stage == 0:
        sum_a, sum_b, sum_c, sum_d, leg_ref, adj_ref, res_ref, *refs = refs
    else:
        sum_a, sum_b, sum_c, sum_d, leg_ref, adj_ref, res_ref, last_ref, past_ref, *refs = refs
    new_ref, along_ref, out_ref, norm_ref, hist_ref, acc_ref = refs
    norm, product = sums_of((sum_a, sum_b, sum_c, sum_d), chunk_rows)
    hist_ref[...] = jnp.zeros_like(hist_ref)
    if stage == 0:
        alpha = norm / product
        beta = jnp.zeros_like(norm)
        hist_ref[2:3, :] = scalar_row(alpha)
    else:
        beta = norm / past_ref[0:1, 0:1]
        alpha = norm / (product - beta * norm / past_ref[1:2, 0:1])
        hist_ref[2:3, :] = past_ref[2:3, :]
        hist_ref[3:4, :] = scalar_row(alpha)
    hist_ref[0:1, :] = scalar_row(norm)
    hist_ref[1:2, :] = scalar_row(alpha)
    hist_ref[4:5, :] = scalar_row(beta)
    norm_ref[...] = jnp.zeros_like(norm_ref)

    def step(slot, carry):
        alpha = hist_ref[1:2, :]
        beta = hist_ref[4:5, :]
        parts = []
        for tile in range(leg_ref.shape[1] // LANES):
            cols = slice(tile * LANES, (tile + 1) * LANES)
            res = res_ref[slot, :, cols]
            along = res + adj_ref[slot, :, cols]
            if stage > 0:
                along = along + beta * last_ref[slot, :, cols]
            along_ref[slot, :, cols] = along
            part = res - alpha * along
            new_ref[slot, :, cols] = part
            parts.append(part)
        norm_ref[...] += square_sum(parts)
        forward(jnp.concatenate(parts, axis=1), leg_ref, acc_ref, slot, slots, chunk_rows)
        return carry

    lax.fori_loop(0, slots, step, 0, unroll=UNROLL)
    out_ref[...] = acc_ref[...].astype(BF16)


def last_kernel(slots, chunk_rows, *refs):
    sum_a, sum_b, sum_c, sum_d, adj_ref, res0_ref, res1_ref, res2_ref, last_ref, past_ref, *refs = refs
    sol_hbm, fin_hbm, turn_ref, sol_ref, fin_ref, sol_sems, fin_sems = refs
    norm, product = sums_of((sum_a, sum_b, sum_c, sum_d), chunk_rows)
    beta = norm / past_ref[0:1, 0:1]
    alpha = scalar_row(norm / (product - beta * norm / past_ref[1:2, 0:1]))
    beta = scalar_row(beta)
    alpha0, alpha1, beta1 = past_ref[2:3, :], past_ref[3:4, :], past_ref[4:5, :]
    tiles = adj_ref.shape[2] // LANES
    height = GROUPS * SUB

    rows_each = sol_hbm.shape[0] // slots
    copies = []

    def send(slot):
        rows = pl.ds(slot * rows_each, rows_each)
        copies.append(pltpu.make_async_copy(sol_ref.at[rows], sol_hbm.at[rows], sol_sems.at[slot]))
        copies.append(pltpu.make_async_copy(fin_ref.at[rows], fin_hbm.at[rows], fin_sems.at[slot]))
        copies[-2].start()
        copies[-1].start()

    for slot in range(slots):
        for tile in range(tiles):
            cols = slice(tile * LANES, (tile + 1) * LANES)
            res2 = res2_ref[slot, :, cols]
            along = res2 + adj_ref[slot, :, cols] + beta * last_ref[slot, :, cols]
            first = res0_ref[slot, :, cols]
            second = res1_ref[slot, :, cols] + beta1 * first
            third = res2 + beta * second
            turn_ref[(2 * tile) * height : (2 * tile + 1) * height, :] = res2 - alpha * along
            turn_ref[(2 * tile + 1) * height : (2 * tile + 2) * height, :] = (
                alpha0 * first + alpha1 * second + alpha * third
            )
            for group in range(GROUPS):
                for part in range(2):
                    rows = flat_rows(slot, group, tile, part, tiles)
                    at = group * SUB + part
                    fin_ref[rows, :] = turn_ref[pl.ds((2 * tile) * height + at, SHARES, stride=2), :]
                    sol_ref[rows, :] = turn_ref[pl.ds((2 * tile + 1) * height + at, SHARES, stride=2), :]
        if slot > 0:
            send(slot - 1)
    send(slots - 1)
    for copy in copies:
        copy.wait()


def fourier_kernel(chunk_rows, slots, norm_factor, map_ref, out_ref, column_ref, waves_ref):
    rows = 32
    lon_count = out_ref.shape[1]
    blocks = map_ref.shape[0]
    compact = jnp.concatenate([map_ref[...].astype(F32), jnp.zeros((SUB - blocks, LANES), F32)], axis=0)
    columns = jnp.concatenate([compact, jnp.zeros((LANES - SUB, LANES), F32)], axis=0).T
    for block in range(blocks):
        column_ref[block * LANES : (block + 1) * LANES, :] = jnp.broadcast_to(
            columns[:, block : block + 1], (LANES, LANES)
        )
    for band in range(waves_ref.shape[0] // chunk_rows):
        wave = column_ref[band * slots : (band + 1) * slots, :]
        for part in range(2):
            at = band * chunk_rows + part * slots
            waves_ref[at : at + slots, :] = wave
    lane = lax.broadcasted_iota(jnp.int32, (rows, LANES), 1).astype(F32)
    local = lax.broadcasted_iota(jnp.int32, (rows, LANES), 0)

    def step(index, carry):
        at = pl.multiple_of(index * rows, rows)
        wave = waves_ref[pl.ds(at, rows), :]
        row = (local + at).astype(F32)
        within = row - chunk_rows * jnp.floor((row + 0.5) * (1.0 / chunk_rows))
        quarter = jnp.where(within > slots - 0.5, 0.25 * lon_count, 0.0)
        cosine, sine = turn(wave * lane + quarter, lon_count)
        step_cos, step_sin = turn(wave * float(LANES), lon_count)
        before = (cosine * step_cos + sine * step_sin) * norm_factor
        now = cosine * norm_factor
        twice = step_cos + step_cos
        for tile in range(lon_count // LANES):
            out_ref[pl.ds(at, rows), tile * LANES : (tile + 1) * LANES] = now.astype(BF16)
            before, now = now, twice * now - before
        return carry

    lax.fori_loop(0, waves_ref.shape[0] // rows, step, 0, unroll=5)


def weight_kernel(*refs):
    *near_refs, out_ref, held_ref = refs
    height = near_refs[0].shape[0]
    for turn_at, near_ref in enumerate(near_refs):
        held_ref[turn_at, :height, :] = near_ref[...]
    share = lax.rem(band_index(), SHARES)
    for place in range(SHARES):
        out_ref[place * height : (place + 1) * height, :] = held_ref[jnp.bitwise_xor(share, place), :height, :]


def turn(phase, period):
    phase = phase - period * jnp.floor(phase * (1.0 / period) + 0.5)
    quadrant = jnp.floor(phase * (4.0 / period) + 0.5)
    angle = (phase - quadrant * (0.25 * period)) * (2.0 * math.pi / period)
    sq = angle * angle
    cosine = 1.0 + sq * (-1.0 / 2 + sq * (1.0 / 24 + sq * (-1.0 / 720 + sq * (1.0 / 40320))))
    sine = angle * (1.0 + sq * (-1.0 / 6 + sq * (1.0 / 120 + sq * (-1.0 / 5040 + sq * (1.0 / 362880)))))
    odd = jnp.abs(quadrant) == 1.0
    cos_base = jnp.where(odd, -quadrant * sine, cosine)
    sin_base = jnp.where(odd, quadrant * cosine, sine)
    back = jnp.abs(quadrant) == 2.0
    return jnp.where(back, -cos_base, cos_base), jnp.where(back, -sin_base, sin_base)


def pieces_of(value):
    high = value.astype(BF16).astype(F32)
    middle = (value - high).astype(BF16).astype(F32)
    low = (value - high - middle).astype(BF16).astype(F32)
    return high, middle, low


def grid_kernel(x_ref, table_ref, weight_ref, norm_ref, out_ref, turned_ref, wide_ref):
    count, lons = table_ref.shape
    step = 256
    turned_ref[...] = x_ref[...].T
    energy = jnp.zeros((SUB, step), F32)
    for first in range(0, lons, step):
        cols = slice(first, first + step)
        grid = jnp.dot(turned_ref[...], table_ref[:, cols], preferred_element_type=F32)
        weight = weight_ref[:, cols]
        weighted = []
        for group in range(GROUPS):
            rows = grid[group * PIECE : (group + 1) * PIECE]
            product = weight * rows
            weighted.append(product)
            square = product * rows
            for block in range(0, PIECE, SUB):
                energy = energy + square[block : block + SUB]
        weighted.append(jnp.zeros((LANES - SPARE, step), F32))
        wide_ref[:, cols] = jnp.concatenate(weighted, axis=0).astype(BF16)
    lane = lane_of(1)
    spare = jnp.zeros((1, LANES), F32)
    values = pieces_of(jnp.sum(norm_ref[...], axis=(0, 1), keepdims=True))
    values = values + pieces_of(jnp.sum(energy, axis=(0, 1), keepdims=True))
    for place, value in enumerate(values):
        spare = jnp.where(lane == SPARE + place, value, spare)
    for first in range(0, count, step):
        rows = slice(first, first + step)
        back = lax.dot_general(
            table_ref[rows, :], wide_ref[...], (((1,), (1,)), ((), ())), preferred_element_type=F32
        )
        out_ref[rows, :] = jnp.where(lane >= SPARE, spare, back).astype(BF16)


def tail_kernel(x_ref, out_ref):
    total = jnp.zeros((SUB, LANES), F32)
    block = 2 * SUB
    for first in range(0, x_ref.shape[0], block):
        value = x_ref[first : first + block, :].astype(F32)
        total = total + value[:SUB] + value[SUB:]
    out_ref[...] = total


def exchange(payload, parts):
    rows = payload.shape[0]
    packed = payload.reshape(parts, rows // parts // 2, 2, LANES)
    return lax.all_to_all(packed, BAND, 0, 0, tiled=True).reshape(rows, LANES)


def call(kernel, name, outs, ins, scratch=(), vmem=24, flops=2_000_000_000, place=pltpu.VMEM):
    return pl.pallas_call(
        kernel,
        in_specs=ins,
        out_specs=[pl.BlockSpec(memory_space=place)] * len(outs),
        out_shape=outs,
        scratch_shapes=scratch,
        compiler_params=pltpu.CompilerParams(vmem_limit_bytes=vmem * 1024 * 1024),
        cost_estimate=pl.CostEstimate(flops=flops, bytes_accessed=1_000_000, transcendentals=0),
        name=name,
    )


def on_device(right_side, legendre, wave_map, obs_weight):
    slots, degrees, lats = legendre.shape
    lon_count = obs_weight.shape[1]
    bands = ZS * YS * CS
    rows = bands * 2 * slots
    chunk_rows = 2 * slots
    smem = pl.BlockSpec(memory_space=pltpu.SMEM)
    vmem = pl.BlockSpec(memory_space=pltpu.VMEM)
    flat = right_side.reshape(-1, LANES)
    vec_shape = jax.ShapeDtypeStruct((slots, GROUPS * SUB, degrees), F32)
    payload_shape = jax.ShapeDtypeStruct((rows, LANES), BF16)
    small_shape = jax.ShapeDtypeStruct((SUB, LANES), F32)
    flat_shape = jax.ShapeDtypeStruct(flat.shape, F32)
    held = pltpu.VMEM((rows, LANES), F32)

    (table,) = call(
        functools.partial(fourier_kernel, chunk_rows, slots, 1.0 / math.sqrt(wave_map.shape[0])),
        "fourier",
        [jax.ShapeDtypeStruct((rows, lon_count), BF16)],
        [vmem],
        [pltpu.VMEM((wave_map.shape[0], LANES), F32), pltpu.VMEM((rows, LANES), F32)],
        flops=4_000_000_000,
    )(wave_map.reshape(-1, LANES))
    flat, table = lax.optimization_barrier((flat, table))

    res, payload, norm = call(
        functools.partial(first_kernel, slots, chunk_rows),
        "first",
        [vec_shape, payload_shape, small_shape],
        [smem, vmem, vmem],
        [held, pltpu.VMEM((GROUPS * SUB, LANES), F32)],
    )(wave_map, flat, legendre)

    near = [obs_weight]
    for turn_at in range(1, SHARES):
        pairs = [(at, at ^ turn_at) for at in range(YS * CS)]
        near.append(lax.ppermute(obs_weight, ("y", "c"), pairs))
    (weight,) = call(
        weight_kernel,
        "weight",
        [jax.ShapeDtypeStruct((PIECE, lon_count), F32)],
        [vmem] * SHARES,
        [pltpu.VMEM((SHARES, 2 * SUB, lon_count), F32)],
    )(*near)
    payload, table, weight = lax.optimization_barrier((payload, table, weight))

    def reach(payload, norm):
        arrived = exchange(payload, bands)
        (back,) = call(
            grid_kernel,
            "grid",
            [payload_shape],
            [vmem] * 4,
            [pltpu.VMEM((LANES, rows), BF16), pltpu.VMEM((LANES, lon_count), BF16)],
        )(arrived, table, weight, norm)
        home = exchange(back, bands)
        (sums,) = call(tail_kernel, "tail", [small_shape], [vmem])(home)
        others = [lax.ppermute(sums, "x", [(i, i ^ k) for i in range(XS)]) for k in range(1, XS)]
        (adjoint,) = call(
            functools.partial(back_kernel, slots, chunk_rows),
            "back",
            [vec_shape],
            [smem, vmem, vmem],
            [held],
            flops=8_000_000_000,
        )(wave_map, home, legendre)
        return adjoint, [sums] + others

    residuals = [res]
    carried = []
    for stage in range(2):
        adjoint, sums = reach(payload, norm)
        operands = [*sums, legendre, adjoint, residuals[-1], *carried]
        res, along, payload, norm, past = call(
            functools.partial(middle_kernel, stage, slots, chunk_rows),
            f"middle{stage}",
            [vec_shape, vec_shape, payload_shape, small_shape, small_shape],
            [vmem] * len(operands),
            [held],
        )(*operands)
        residuals.append(res)
        carried = [along, past]
    adjoint, sums = reach(payload, norm)
    solution, residual = call(
        functools.partial(last_kernel, slots, chunk_rows),
        "last",
        [flat_shape, flat_shape],
        [vmem] * 10,
        [
            pltpu.VMEM((2 * GROUPS * SUB * (degrees // LANES), LANES), F32),
            pltpu.VMEM(flat.shape, F32),
            pltpu.VMEM(flat.shape, F32),
            pltpu.SemaphoreType.DMA((slots,)),
            pltpu.SemaphoreType.DMA((slots,)),
        ],
        place=pltpu.HBM,
    )(*sums, adjoint, *residuals, along, past)
    return solution.reshape(right_side.shape), residual.reshape(right_side.shape)


def solution(mesh):
    split = Mesh(mesh.devices.reshape(ZS, YS, CS, XS), ("z", "y", "c", "x"))
    return jax.shard_map(
        on_device,
        mesh=split,
        in_specs=(P(BAND, None, "x", None, None), P(BAND, None, None), P(), P(BAND, None)),
        out_specs=(P(BAND, None, "x", None, None), P(BAND, None, "x", None, None)),
        check_vma=False,
    )
```

```python
import functools
import math

import jax
import jax.numpy as jnp
from jax import lax
from jax.experimental import pallas as pl
from jax.experimental.pallas import tpu as pltpu
from jax.sharding import Mesh
from jax.sharding import PartitionSpec as P

ZS, YS, CS, XS = 8, 4, 2, 4
BAND = ("z", "y", "c")
GROUPS = 3
SHARES = 4
PIECE = 40
PIECES = 16
SUB = 8
LANES = 128
SPARE = GROUPS * PIECE
F32 = jnp.float32
BF16 = jnp.bfloat16
UNROLL = 10


def lane_of(rows=SUB):
    return lax.broadcasted_iota(jnp.int32, (rows, LANES), 1)


def scatter_rows(value, acc_ref, slot, chunk_rows, slots):
    lane = lane_of()
    for piece in range(PIECES):
        first = piece * PIECE
        tile, offset = first // LANES, first % LANES
        out = jnp.zeros((SUB, LANES), F32)
        for group in reversed(range(GROUPS)):
            rows = slice(group * SUB, (group + 1) * SUB)
            source = value[rows, tile * LANES : (tile + 1) * LANES]
            if offset + PIECE > LANES:
                following = value[rows, (tile + 1) * LANES : (tile + 2) * LANES]
                source = jnp.where(lane >= offset, source, following)
            shift = (group * PIECE - offset) % LANES
            if shift:
                source = pltpu.roll(source, shift, 1)
            out = jnp.where(lane < (group + 1) * PIECE, source, out)
        acc_ref[pl.ds(piece * SHARES * chunk_rows + slot, SUB, stride=slots), :] = out


def gather_rows(held_ref, slot, chunk_rows, slots, lat_tiles):
    lane = lane_of()
    tiles = [[None] * lat_tiles for _ in range(GROUPS)]
    for piece in range(PIECES):
        first = piece * PIECE
        tile, offset = first // LANES, first % LANES
        rows = held_ref[pl.ds(piece * SHARES * chunk_rows + slot, SUB, stride=slots), :]
        for group in range(GROUPS):
            shift = (offset - group * PIECE) % LANES
            moved = pltpu.roll(rows, shift, 1) if shift else rows
            known = tiles[group][tile]
            tiles[group][tile] = moved if known is None else jnp.where(lane >= offset, moved, known)
            if offset + PIECE > LANES:
                tiles[group][tile + 1] = moved
    return jnp.concatenate([jnp.concatenate(row, axis=1) for row in tiles], axis=0)


def square_sum(parts):
    total = None
    for part in parts:
        for group in range(GROUPS):
            block = part[group * SUB : (group + 1) * SUB, :]
            total = block * block if total is None else total + block * block
    return total


def triangle_tile(wave, tile):
    return lane_of(GROUPS * SUB) + tile * LANES >= wave


def band_index():
    return (lax.axis_index("z") * YS + lax.axis_index("y")) * CS + lax.axis_index("c")


def wave_of(waves_ref, slots, slot):
    return waves_ref[band_index() * slots + slot]


def flat_rows(slot, group, tile, part, tiles):
    first = ((slot * 2 + part) * GROUPS + group) * SHARES * tiles + tile
    return pl.ds(first, SHARES, stride=tiles)


def first_kernel(slots, chunk_rows, waves_ref, vec_ref, leg_ref, res_ref, out_ref, norm_ref, acc_ref, turn_ref):
    tiles = leg_ref.shape[1] // LANES
    norm_ref[...] = jnp.zeros_like(norm_ref)

    def step(slot, carry):
        wave = wave_of(waves_ref, slots, slot)
        parts = []
        for tile in range(tiles):
            cols = slice(tile * LANES, (tile + 1) * LANES)
            for group in range(GROUPS):
                for part in range(2):
                    rows = vec_ref[flat_rows(slot, group, tile, part, tiles), :]
                    turn_ref[pl.ds(group * SUB + part, SHARES, stride=2), :] = rows
            parts.append(jnp.where(triangle_tile(wave, tile), turn_ref[...], 0.0))
            res_ref[slot, :, cols] = parts[-1]
        norm_ref[...] += square_sum(parts)
        forward(jnp.concatenate(parts, axis=1), leg_ref, acc_ref, slot, slots, chunk_rows)
        return carry

    lax.fori_loop(0, slots, step, 0, unroll=UNROLL)
    out_ref[...] = acc_ref[...].astype(BF16)


def forward(vector, leg_ref, acc_ref, slot, slots, chunk_rows):
    coeffs = jnp.dot(vector.astype(BF16), leg_ref[slot], preferred_element_type=F32)
    scatter_rows(coeffs, acc_ref, slot, chunk_rows, slots)


def sums_of(sum_refs, chunk_rows):
    total = sum_refs[0][...]
    for ref in sum_refs[1:]:
        total = total + ref[...]
    total = total * (1.0 / chunk_rows)
    lane = lane_of()
    norm = jnp.sum(jnp.where((lane >= SPARE) & (lane < SPARE + 3), total, 0.0), axis=(0, 1), keepdims=True)
    energy = jnp.sum(jnp.where((lane >= SPARE + 3) & (lane < SPARE + 6), total, 0.0), axis=(0, 1), keepdims=True)
    return norm, norm + energy


def back_kernel(slots, chunk_rows, waves_ref, home_ref, leg_ref, adj_ref, held_ref):
    held_ref[...] = home_ref[...].astype(F32)
    tiles = leg_ref.shape[2] // LANES

    def step(slot, carry):
        wave = wave_of(waves_ref, slots, slot)
        home = gather_rows(held_ref, slot, chunk_rows, slots, tiles).astype(BF16)
        adjoint = lax.dot_general(home, leg_ref[slot], (((1,), (1,)), ((), ())), preferred_element_type=F32)
        for tile in range(leg_ref.shape[1] // LANES):
            cols = slice(tile * LANES, (tile + 1) * LANES)
            adj_ref[slot, :, cols] = jnp.where(triangle_tile(wave, tile), adjoint[:, cols], 0.0)
        return carry

    lax.fori_loop(0, slots, step, 0, unroll=UNROLL)


def scalar_row(value):
    return jnp.broadcast_to(value, (1, LANES))


def middle_kernel(stage, slots, chunk_rows, *refs):
    if stage == 0:
        sum_a, sum_b, sum_c, sum_d, leg_ref, adj_ref, res_ref, *refs = refs
    else:
        sum_a, sum_b, sum_c, sum_d, leg_ref, adj_ref, res_ref, last_ref, past_ref, *refs = refs
    new_ref, along_ref, out_ref, norm_ref, hist_ref, acc_ref = refs
    norm, product = sums_of((sum_a, sum_b, sum_c, sum_d), chunk_rows)
    hist_ref[...] = jnp.zeros_like(hist_ref)
    if stage == 0:
        alpha = norm / product
        beta = jnp.zeros_like(norm)
        hist_ref[2:3, :] = scalar_row(alpha)
    else:
        beta = norm / past_ref[0:1, 0:1]
        alpha = norm / (product - beta * norm / past_ref[1:2, 0:1])
        hist_ref[2:3, :] = past_ref[2:3, :]
        hist_ref[3:4, :] = scalar_row(alpha)
    hist_ref[0:1, :] = scalar_row(norm)
    hist_ref[1:2, :] = scalar_row(alpha)
    hist_ref[4:5, :] = scalar_row(beta)
    norm_ref[...] = jnp.zeros_like(norm_ref)

    def step(slot, carry):
        alpha = hist_ref[1:2, :]
        beta = hist_ref[4:5, :]
        parts = []
        for tile in range(leg_ref.shape[1] // LANES):
            cols = slice(tile * LANES, (tile + 1) * LANES)
            res = res_ref[slot, :, cols]
            along = res + adj_ref[slot, :, cols]
            if stage > 0:
                along = along + beta * last_ref[slot, :, cols]
            along_ref[slot, :, cols] = along
            part = res - alpha * along
            new_ref[slot, :, cols] = part
            parts.append(part)
        norm_ref[...] += square_sum(parts)
        forward(jnp.concatenate(parts, axis=1), leg_ref, acc_ref, slot, slots, chunk_rows)
        return carry

    lax.fori_loop(0, slots, step, 0, unroll=UNROLL)
    out_ref[...] = acc_ref[...].astype(BF16)


def last_kernel(slots, chunk_rows, *refs):
    sum_a, sum_b, sum_c, sum_d, adj_ref, res0_ref, res1_ref, res2_ref, last_ref, past_ref, *refs = refs
    sol_hbm, fin_hbm, turn_ref, sol_ref, fin_ref, sol_sems, fin_sems = refs
    norm, product = sums_of((sum_a, sum_b, sum_c, sum_d), chunk_rows)
    beta = norm / past_ref[0:1, 0:1]
    alpha = scalar_row(norm / (product - beta * norm / past_ref[1:2, 0:1]))
    beta = scalar_row(beta)
    alpha0, alpha1, beta1 = past_ref[2:3, :], past_ref[3:4, :], past_ref[4:5, :]
    tiles = adj_ref.shape[2] // LANES
    height = GROUPS * SUB

    rows_each = sol_hbm.shape[0] // slots
    copies = []

    def send(slot):
        rows = pl.ds(slot * rows_each, rows_each)
        copies.append(pltpu.make_async_copy(sol_ref.at[rows], sol_hbm.at[rows], sol_sems.at[slot]))
        copies.append(pltpu.make_async_copy(fin_ref.at[rows], fin_hbm.at[rows], fin_sems.at[slot]))
        copies[-2].start()
        copies[-1].start()

    for slot in range(slots):
        for tile in range(tiles):
            cols = slice(tile * LANES, (tile + 1) * LANES)
            res2 = res2_ref[slot, :, cols]
            along = res2 + adj_ref[slot, :, cols] + beta * last_ref[slot, :, cols]
            first = res0_ref[slot, :, cols]
            second = res1_ref[slot, :, cols] + beta1 * first
            third = res2 + beta * second
            turn_ref[(2 * tile) * height : (2 * tile + 1) * height, :] = res2 - alpha * along
            turn_ref[(2 * tile + 1) * height : (2 * tile + 2) * height, :] = (
                alpha0 * first + alpha1 * second + alpha * third
            )
            for group in range(GROUPS):
                for part in range(2):
                    rows = flat_rows(slot, group, tile, part, tiles)
                    at = group * SUB + part
                    fin_ref[rows, :] = turn_ref[pl.ds((2 * tile) * height + at, SHARES, stride=2), :]
                    sol_ref[rows, :] = turn_ref[pl.ds((2 * tile + 1) * height + at, SHARES, stride=2), :]
        if slot > 0:
            send(slot - 1)
    send(slots - 1)
    for copy in copies:
        copy.wait()


def fourier_kernel(chunk_rows, slots, norm_factor, map_ref, out_ref, column_ref, waves_ref):
    rows = 32
    lon_count = out_ref.shape[1]
    blocks = map_ref.shape[0]
    compact = jnp.concatenate([map_ref[...].astype(F32), jnp.zeros((SUB - blocks, LANES), F32)], axis=0)
    columns = jnp.concatenate([compact, jnp.zeros((LANES - SUB, LANES), F32)], axis=0).T
    for block in range(blocks):
        column_ref[block * LANES : (block + 1) * LANES, :] = jnp.broadcast_to(
            columns[:, block : block + 1], (LANES, LANES)
        )
    for band in range(waves_ref.shape[0] // chunk_rows):
        wave = column_ref[band * slots : (band + 1) * slots, :]
        for part in range(2):
            at = band * chunk_rows + part * slots
            waves_ref[at : at + slots, :] = wave
    lane = lax.broadcasted_iota(jnp.int32, (rows, LANES), 1).astype(F32)
    local = lax.broadcasted_iota(jnp.int32, (rows, LANES), 0)

    def step(index, carry):
        at = pl.multiple_of(index * rows, rows)
        wave = waves_ref[pl.ds(at, rows), :]
        row = (local + at).astype(F32)
        within = row - chunk_rows * jnp.floor((row + 0.5) * (1.0 / chunk_rows))
        quarter = jnp.where(within > slots - 0.5, 0.25 * lon_count, 0.0)
        cosine, sine = turn(wave * lane + quarter, lon_count)
        step_cos, step_sin = turn(wave * float(LANES), lon_count)
        before = (cosine * step_cos + sine * step_sin) * norm_factor
        now = cosine * norm_factor
        twice = step_cos + step_cos
        for tile in range(lon_count // LANES):
            out_ref[pl.ds(at, rows), tile * LANES : (tile + 1) * LANES] = now.astype(BF16)
            before, now = now, twice * now - before
        return carry

    lax.fori_loop(0, waves_ref.shape[0] // rows, step, 0, unroll=5)


def weight_kernel(*refs):
    *near_refs, out_ref, held_ref = refs
    height = near_refs[0].shape[0]
    for turn_at, near_ref in enumerate(near_refs):
        held_ref[turn_at, :height, :] = near_ref[...]
    share = lax.rem(band_index(), SHARES)
    for place in range(SHARES):
        out_ref[place * height : (place + 1) * height, :] = held_ref[jnp.bitwise_xor(share, place), :height, :]


def turn(phase, period):
    phase = phase - period * jnp.floor(phase * (1.0 / period) + 0.5)
    quadrant = jnp.floor(phase * (4.0 / period) + 0.5)
    angle = (phase - quadrant * (0.25 * period)) * (2.0 * math.pi / period)
    sq = angle * angle
    cosine = 1.0 + sq * (-1.0 / 2 + sq * (1.0 / 24 + sq * (-1.0 / 720 + sq * (1.0 / 40320))))
    sine = angle * (1.0 + sq * (-1.0 / 6 + sq * (1.0 / 120 + sq * (-1.0 / 5040 + sq * (1.0 / 362880)))))
    odd = jnp.abs(quadrant) == 1.0
    cos_base = jnp.where(odd, -quadrant * sine, cosine)
    sin_base = jnp.where(odd, quadrant * cosine, sine)
    back = jnp.abs(quadrant) == 2.0
    return jnp.where(back, -cos_base, cos_base), jnp.where(back, -sin_base, sin_base)


def pieces_of(value):
    high = value.astype(BF16).astype(F32)
    middle = (value - high).astype(BF16).astype(F32)
    low = (value - high - middle).astype(BF16).astype(F32)
    return high, middle, low


def grid_kernel(x_ref, table_ref, weight_ref, norm_ref, out_ref, turned_ref, wide_ref):
    count, lons = table_ref.shape
    step = 640
    turned_ref[...] = x_ref[...].T
    energy = jnp.zeros((SUB, step), F32)
    for first in range(0, lons, step):
        cols = slice(first, first + step)
        grid = jnp.dot(turned_ref[...], table_ref[:, cols], preferred_element_type=F32)
        weight = weight_ref[:, cols]
        weighted = []
        for group in range(GROUPS):
            rows = grid[group * PIECE : (group + 1) * PIECE]
            product = weight * rows
            weighted.append(product)
            square = product * rows
            for block in range(0, PIECE, SUB):
                energy = energy + square[block : block + SUB]
        weighted.append(jnp.zeros((LANES - SPARE, step), F32))
        wide_ref[:, cols] = jnp.concatenate(weighted, axis=0).astype(BF16)
    lane = lane_of(1)
    spare = jnp.zeros((1, LANES), F32)
    values = pieces_of(jnp.sum(norm_ref[...], axis=(0, 1), keepdims=True))
    values = values + pieces_of(jnp.sum(energy, axis=(0, 1), keepdims=True))
    for place, value in enumerate(values):
        spare = jnp.where(lane == SPARE + place, value, spare)
    for first in range(0, count, step):
        rows = slice(first, first + step)
        back = lax.dot_general(
            table_ref[rows, :], wide_ref[...], (((1,), (1,)), ((), ())), preferred_element_type=F32
        )
        out_ref[rows, :] = jnp.where(lane >= SPARE, spare, back).astype(BF16)


def tail_kernel(x_ref, out_ref):
    total = jnp.zeros((SUB, LANES), F32)
    block = 2 * SUB
    for first in range(0, x_ref.shape[0], block):
        value = x_ref[first : first + block, :].astype(F32)
        total = total + value[:SUB] + value[SUB:]
    out_ref[...] = total


def exchange(payload, parts):
    rows = payload.shape[0]
    packed = payload.reshape(parts, rows // parts // 4, 4, LANES)
    return lax.all_to_all(packed, BAND, 0, 0, tiled=True).reshape(rows, LANES)


def call(kernel, name, outs, ins, scratch=(), vmem=24, flops=2_000_000_000, place=pltpu.VMEM):
    return pl.pallas_call(
        kernel,
        in_specs=ins,
        out_specs=[pl.BlockSpec(memory_space=place)] * len(outs),
        out_shape=outs,
        scratch_shapes=scratch,
        compiler_params=pltpu.CompilerParams(vmem_limit_bytes=vmem * 1024 * 1024),
        cost_estimate=pl.CostEstimate(flops=flops, bytes_accessed=1_000_000, transcendentals=0),
        name=name,
    )


def on_device(right_side, legendre, wave_map, obs_weight):
    slots, degrees, lats = legendre.shape
    lon_count = obs_weight.shape[1]
    bands = ZS * YS * CS
    rows = bands * 2 * slots
    chunk_rows = 2 * slots
    smem = pl.BlockSpec(memory_space=pltpu.SMEM)
    vmem = pl.BlockSpec(memory_space=pltpu.VMEM)
    flat = right_side.reshape(-1, LANES)
    vec_shape = jax.ShapeDtypeStruct((slots, GROUPS * SUB, degrees), F32)
    payload_shape = jax.ShapeDtypeStruct((rows, LANES), BF16)
    small_shape = jax.ShapeDtypeStruct((SUB, LANES), F32)
    flat_shape = jax.ShapeDtypeStruct(flat.shape, F32)
    held = pltpu.VMEM((rows, LANES), F32)

    (table,) = call(
        functools.partial(fourier_kernel, chunk_rows, slots, 1.0 / math.sqrt(wave_map.shape[0])),
        "fourier",
        [jax.ShapeDtypeStruct((rows, lon_count), BF16)],
        [vmem],
        [pltpu.VMEM((wave_map.shape[0], LANES), F32), pltpu.VMEM((rows, LANES), F32)],
        flops=4_000_000_000,
    )(wave_map.reshape(-1, LANES))
    flat, table = lax.optimization_barrier((flat, table))

    res, payload, norm = call(
        functools.partial(first_kernel, slots, chunk_rows),
        "first",
        [vec_shape, payload_shape, small_shape],
        [smem, vmem, vmem],
        [held, pltpu.VMEM((GROUPS * SUB, LANES), F32)],
    )(wave_map, flat, legendre)

    near = [obs_weight]
    for turn_at in range(1, SHARES):
        pairs = [(at, at ^ turn_at) for at in range(YS * CS)]
        near.append(lax.ppermute(obs_weight, ("y", "c"), pairs))
    (weight,) = call(
        weight_kernel,
        "weight",
        [jax.ShapeDtypeStruct((PIECE, lon_count), F32)],
        [vmem] * SHARES,
        [pltpu.VMEM((SHARES, 2 * SUB, lon_count), F32)],
    )(*near)
    payload, table, weight = lax.optimization_barrier((payload, table, weight))

    def reach(payload, norm):
        arrived = exchange(payload, bands)
        (back,) = call(
            grid_kernel,
            "grid",
            [payload_shape],
            [vmem] * 4,
            [pltpu.VMEM((LANES, rows), BF16), pltpu.VMEM((LANES, lon_count), BF16)],
        )(arrived, table, weight, norm)
        home = exchange(back, bands)
        (sums,) = call(tail_kernel, "tail", [small_shape], [vmem])(home)
        others = [lax.ppermute(sums, "x", [(i, i ^ k) for i in range(XS)]) for k in range(1, XS)]
        (adjoint,) = call(
            functools.partial(back_kernel, slots, chunk_rows),
            "back",
            [vec_shape],
            [smem, vmem, vmem],
            [held],
            flops=8_000_000_000,
        )(wave_map, home, legendre)
        return adjoint, [sums] + others

    residuals = [res]
    carried = []
    for stage in range(2):
        adjoint, sums = reach(payload, norm)
        operands = [*sums, legendre, adjoint, residuals[-1], *carried]
        res, along, payload, norm, past = call(
            functools.partial(middle_kernel, stage, slots, chunk_rows),
            f"middle{stage}",
            [vec_shape, vec_shape, payload_shape, small_shape, small_shape],
            [vmem] * len(operands),
            [held],
        )(*operands)
        residuals.append(res)
        carried = [along, past]
    adjoint, sums = reach(payload, norm)
    solution, residual = call(
        functools.partial(last_kernel, slots, chunk_rows),
        "last",
        [flat_shape, flat_shape],
        [vmem] * 10,
        [
            pltpu.VMEM((2 * GROUPS * SUB * (degrees // LANES), LANES), F32),
            pltpu.VMEM(flat.shape, F32),
            pltpu.VMEM(flat.shape, F32),
            pltpu.SemaphoreType.DMA((slots,)),
            pltpu.SemaphoreType.DMA((slots,)),
        ],
        place=pltpu.HBM,
    )(*sums, adjoint, *residuals, along, past)
    return solution.reshape(right_side.shape), residual.reshape(right_side.shape)


def solution(mesh):
    split = Mesh(mesh.devices.reshape(ZS, YS, CS, XS), ("z", "y", "c", "x"))
    return jax.shard_map(
        on_device,
        mesh=split,
        in_specs=(P(BAND, None, "x", None, None), P(BAND, None, None), P(), P(BAND, None)),
        out_specs=(P(BAND, None, "x", None, None), P(BAND, None, "x", None, None)),
        check_vma=False,
    )
```
